256 devices in a mesh: ta: 8 (over z_lo, x), ha: 4 (over y), wa: 8 (over z_hi, core).
Axes of the slice: x: 4, y: 4, z: 8 (z_hi: 4, z_lo: 2; z = z_hi * 2 + z_lo), core: 2. Of those that a mesh axis runs over, the one named last changes fastest.
Arguments:
- volume: bfloat16 [8, 128, 128, 128], P('ta', 'ha', 'wa'), may hold values from -6 to 6
- cotangent: bfloat16 [8, 128, 128, 128], P('ta', 'ha', 'wa'), may hold values from -6 to 6
- kernel_one: bfloat16 [3, 3, 3, 128, 128], replicated, may hold values from -0.109375 to 0.109375
- kernel_two: bfloat16 [3, 3, 3, 128, 128], replicated, may hold values from -0.109375 to 0.109375
Outputs:
- d_volume: bfloat16 [8, 128, 128, 128], P('ta', 'ha', 'wa')
- grad_one: float32 [3, 3, 3, 128, 128], replicated
- grad_two: float32 [3, 3, 3, 128, 128], replicated
The draws below stay inside these ranges and needn't reach their ends.
All inputs are finite; a program needn't handle non-finite values.
Results may differ from the reference program's by a relative error of at most 0.0049.
Values may be sent and summed in bfloat16 or wider, within the bound.
A program may use at most 64 MiB of HBM per device.

```python
import jax
import jax.numpy as jnp
from jax import lax

CHANNELS = 128
FRAMES = 8
HEIGHT = 128
WIDTH_ALL = 128


def steps_of(rng, dims, shards, smallest, high):
    gain, own = 1.0, jax.random.fold_in(rng, 6)
    for dim, blocks in shards:
        draws = jnp.exp(jax.random.uniform(jax.random.fold_in(own, dim), (blocks,), jnp.float32, smallest / len(shards), high / len(shards)))
        gain = gain * jnp.repeat(draws, dims[dim] // blocks).reshape([-1 if axis == dim else 1 for axis in range(len(dims))])
    return gain


def centred(own_key, extent, spread, reach, split=(), dtype=jnp.bfloat16):
    array = spread * jax.random.normal(own_key, extent, jnp.float32)
    if split:
        array = array * steps_of(own_key, extent, split, -0.22, 0.18)
    return jnp.clip(array, -reach, reach).astype(dtype)


def setup_inputs(seed: int = 0) -> dict:
    splits = jax.random.split(jax.random.key(seed), 5)
    volume = centred(splits[0], (FRAMES, HEIGHT, WIDTH_ALL, CHANNELS), 1.0, 6.0, ((0, 8), (1, 4), (2, 8)))
    cotangent = centred(splits[1], (FRAMES, HEIGHT, WIDTH_ALL, CHANNELS), 1.0, 6.0, ((0, 8), (1, 4), (2, 8)))
    kernel_one = centred(splits[2], (3, 3, 3, CHANNELS, CHANNELS), (27 * CHANNELS) ** -0.5, 0.109375)
    kernel_two = centred(splits[3], (3, 3, 3, CHANNELS, CHANNELS), (27 * CHANNELS) ** -0.5, 0.109375)
    return {"volume": volume, "cotangent": cotangent, "kernel_one": kernel_one, "kernel_two": kernel_two}


def flip_swap(kernel):
    return jnp.swapaxes(kernel[::-1, ::-1, ::-1], 3, 4)

def pad_field(field):
    return jnp.pad(field.astype(jnp.float32), ((1, 1), (1, 1), (1, 1), (0, 0)))

def conv_full(field, kernel):
    frames, height, width, chans = field.shape
    padded = pad_field(field)
    total = jnp.zeros((frames * height * width, chans), jnp.float32)
    for kt in range(3):
        for kh in range(3):
            for kw in range(3):
                piece = padded[kt:kt + frames, kh:kh + height, kw:kw + width].reshape(-1, chans)
                total = total + jnp.dot(piece, kernel[kt, kh, kw].astype(jnp.float32), precision=lax.Precision.HIGHEST)
    return total.reshape(frames, height, width, chans)

def kernel_grad(field, other):
    frames, height, width, chans = field.shape
    padded = pad_field(field)
    right = other.astype(jnp.float32).reshape(-1, chans)
    blocks = []
    for kt in range(3):
        for kh in range(3):
            for kw in range(3):
                piece = padded[kt:kt + frames, kh:kh + height, kw:kw + width].reshape(-1, chans)
                blocks.append(jnp.dot(piece.T, right, precision=lax.Precision.HIGHEST))
    return jnp.stack(blocks).reshape(3, 3, 3, chans, chans)

def reference(volume, cotangent, kernel_one, kernel_two):
    pre = conv_full(volume, kernel_one)
    sig = jax.nn.sigmoid(pre)
    hidden = (pre * sig).astype(jnp.bfloat16)
    d_hidden = conv_full(cotangent, flip_swap(kernel_two))
    d_pre = (d_hidden * sig * (1.0 + pre * (1.0 - sig))).astype(jnp.bfloat16)
    d_volume = conv_full(d_pre, flip_swap(kernel_one)).astype(jnp.bfloat16)
    scale = 1.0 / jnp.sqrt(jnp.float32(FRAMES * HEIGHT * WIDTH_ALL))
    grad_two = kernel_grad(hidden, cotangent) * scale
    grad_one = kernel_grad(volume, d_pre) * scale
    return (d_volume, grad_one, grad_two)
```

```python
import functools

import jax
import jax.numpy as jnp
from jax import lax
from jax.experimental import pallas as pl
from jax.experimental.pallas import tpu as pltpu
from jax.sharding import PartitionSpec as P

MESH = pl.DeviceIdType.MESH
F32 = jnp.float32
BF16 = jnp.bfloat16


def padded_2(cells, sides, width):
    for axis, dim in sides:
        count = lax.axis_size(axis)
        ends = count - 1
        head = lax.slice_in_dim(cells, 0, width, axis=dim)
        tail = lax.slice_in_dim(cells, cells.shape[dim] - width, cells.shape[dim], axis=dim)
        cells = jnp.concatenate(
            [
                lax.ppermute(tail, axis, [(i, (i + 1) % count) for i in range(ends)]),
                cells,
                lax.ppermute(head, axis, [((i + 1) % count, i) for i in range(ends)]),
            ],
            axis=dim,
        )
    return cells


def flip_swap(kernel):
    return jnp.swapaxes(kernel[::-1, ::-1, ::-1], 3, 4)


def window_rows(padded, offset_t, offset_h):
    frames = padded.shape[0] - 2
    height = padded.shape[1] - 2
    width = padded.shape[2] - 2
    chans = padded.shape[3]
    pieces = [
        padded[offset_t : offset_t + frames, offset_h : offset_h + height, shift : shift + width]
        for shift in range(3)
    ]
    return jnp.concatenate(pieces, axis=-1).reshape(-1, 3 * chans)


def conv_local(padded, kernel):
    frames = padded.shape[0] - 2
    height = padded.shape[1] - 2
    width = padded.shape[2] - 2
    chans = padded.shape[3]
    total = jnp.zeros((frames * height * width, chans), jnp.float32)
    for offset_t in range(3):
        for offset_h in range(3):
            rows = window_rows(padded, offset_t, offset_h)
            total = total + jnp.dot(
                rows,
                kernel[offset_t, offset_h].reshape(3 * chans, chans),
                preferred_element_type=jnp.float32,
            )
    return total.reshape(frames, height, width, chans)


def kernel_local(padded, other):
    chans = padded.shape[3]
    right = other.reshape(-1, chans)
    blocks = []
    for offset_t in range(3):
        for offset_h in range(3):
            rows = window_rows(padded, offset_t, offset_h)
            product = lax.dot_general(
                rows, right, (((0,), (0,)), ((), ())), preferred_element_type=jnp.float32
            )
            blocks.append(product.reshape(3, chans, chans))
    return jnp.stack(blocks).reshape(3, 3, 3, chans, chans)


class Place:
    def __init__(self):
        self.ta = lax.axis_index("ta")
        self.ha = lax.axis_index("ha")
        self.wa = lax.axis_index("wa")
        self.core = lax.rem(self.wa, 2)
        self.x = lax.rem(self.ta, 4)
        self.y = self.ha
        self.z = (self.wa // 2) * 2 + self.ta // 4

    def peer_x(self, off):
        to = lax.rem(self.x + off, 4)
        return to, (self.ta - self.x + to, self.ha, self.wa)

    def peer_y(self, off):
        to = lax.rem(self.y + off, 4)
        return to, (self.ta, to, self.wa)

    def peer_z(self, off):
        to = lax.rem(self.z + off, 8)
        return to, (lax.rem(to, 2) * 4 + self.x, self.ha, (to // 2) * 2 + self.core)

    def twin(self):
        return (self.ta, self.ha, self.wa + 1 - 2 * self.core)


def send(src, dst, send_sem, recv_sem, device):
    pltpu.make_async_remote_copy(
        src_ref=src, dst_ref=dst, send_sem=send_sem, recv_sem=recv_sem,
        device_id=device, device_id_type=MESH,
    ).start()


def wait_bytes(ref, sem):
    pltpu.make_async_copy(ref, ref, sem).wait()


PHASES = 8


class Reduce:
    def __init__(self, place, part, full, land0, sums, land1, tops, land2, thirds, land3, lasts, sends, recvs):
        self.at = place
        self.part, self.full = part, full
        self.land0, self.sums, self.land1 = land0, sums, land1
        self.tops, self.land2 = tops, land2
        self.thirds, self.land3, self.lasts = thirds, land3, lasts
        self.sends, self.recvs = sends, recvs

    def first(self, s, off):
        return self.at.peer_x(off) if s == 0 else self.at.peer_y(off)

    def second(self, s, off):
        return self.at.peer_y(off) if s == 0 else self.at.peer_x(off)

    def mine(self, s):
        return (self.at.x, self.at.y) if s == 0 else (self.at.y, self.at.x)

    def pair_send(self):
        other = 4 - 4 * self.at.core
        for s in range(2):
            send(
                self.part.at[pl.ds(other, 4), pl.ds(16 * s, 14)],
                self.land0.at[s],
                self.sends.at[0, s], self.recvs.at[0, s], self.at.twin(),
            )

    def pair_sum(self, s):
        own = 4 * self.at.core
        wait_bytes(self.land0.at[s], self.recvs.at[0, s])

        def step(i, _):
            total = self.part[own + i, pl.ds(16 * s, 14)].astype(F32) + self.land0[s, i].astype(F32)
            self.sums[s, i] = total.astype(BF16)
            return 0

        lax.fori_loop(0, 4, step, 0)

    def first_send(self, s):
        for off in range(1, 4):
            to, device = self.first(s, off)
            send(
                self.sums.at[s, to], self.land1.at[s, off - 1],
                self.sends.at[1, s], self.recvs.at[1, s], device,
            )

    def first_sum(self, s):
        me, _ = self.mine(s)
        wait_bytes(self.land1.at[s], self.recvs.at[1, s])
        total = self.sums[s, me].astype(F32)
        for j in range(3):
            total = total + self.land1[s, j].astype(F32)
        self.tops[s, pl.ds(0, 14)] = total.astype(BF16)
        self.tops[s, pl.ds(14, 2)] = jnp.zeros((2, 16, 128), BF16)

    def second_send(self, s):
        for off in range(1, 4):
            to, device = self.second(s, off)
            send(
                self.tops.at[s, pl.ds(4 * to, 4)], self.land2.at[s, off - 1],
                self.sends.at[2, s], self.recvs.at[2, s], device,
            )

    def second_sum(self, s):
        _, me = self.mine(s)
        wait_bytes(self.land2.at[s], self.recvs.at[2, s])
        total = self.tops[s, pl.ds(4 * me, 4)].astype(F32)
        for j in range(3):
            total = total + self.land2[s, j].astype(F32)
        self.thirds[s] = total.reshape(8, 8, 128)

    def third_send(self, s):
        for off in range(1, 8):
            to, device = self.at.peer_z(off)
            send(
                self.thirds.at[s, to], self.land3.at[s, off - 1],
                self.sends.at[3, s], self.recvs.at[3, s], device,
            )

    def third_sum(self, s):
        wait_bytes(self.land3.at[s], self.recvs.at[3, s])
        total = self.thirds[s, self.at.z]
        for j in range(7):
            total = total + self.land3[s, j]
        self.lasts[s, self.at.z] = total

    def third_gather(self, s):
        for off in range(1, 8):
            _, device = self.at.peer_z(off)
            send(
                self.lasts.at[s, self.at.z], self.lasts.at[s, self.at.z],
                self.sends.at[4, s], self.recvs.at[4, s], device,
            )

    def second_gather(self, s):
        me, me2 = self.mine(s)
        wait_bytes(self.lasts.at[s, pl.ds(0, 7)], self.recvs.at[4, s])
        row = 4 * self.at.core + me
        spot = pl.ds(16 * s + 4 * me2, 4)
        self.full[row, spot] = self.lasts[s].reshape(4, 16, 128).astype(BF16)
        for off in range(1, 4):
            _, device = self.second(s, off)
            send(
                self.full.at[row, spot], self.full.at[row, spot],
                self.sends.at[5, s], self.recvs.at[5, s], device,
            )

    def first_gather(self, s):
        me, me2 = self.mine(s)
        wait_bytes(self.full.at[0, pl.ds(0, 12)], self.recvs.at[5, s])
        row = 4 * self.at.core + me
        spot = pl.ds(16 * s, 14)
        for off in range(1, 4):
            _, device = self.first(s, off)
            send(
                self.full.at[row, spot], self.full.at[row, spot],
                self.sends.at[6, s], self.recvs.at[6, s], device,
            )

    def pair_gather(self, s):
        wait_bytes(self.full.at[pl.ds(0, 3), pl.ds(0, 14)], self.recvs.at[6, s])
        rows = pl.ds(4 * self.at.core, 4)
        spot = pl.ds(16 * s, 14)
        send(
            self.full.at[rows, spot], self.full.at[rows, spot],
            self.sends.at[7, s], self.recvs.at[7, s], self.at.twin(),
        )

    def finish(self, s):
        wait_bytes(self.full.at[pl.ds(0, 4), pl.ds(0, 14)], self.recvs.at[7, s])

    def drain(self, s):
        wait_bytes(self.land0.at[s], self.sends.at[0, s])
        wait_bytes(self.land1.at[s], self.sends.at[1, s])
        wait_bytes(self.land2.at[s], self.sends.at[2, s])
        wait_bytes(self.land3.at[s], self.sends.at[3, s])
        wait_bytes(self.lasts.at[s, pl.ds(0, 7)], self.sends.at[4, s])
        wait_bytes(self.full.at[0, pl.ds(0, 12)], self.sends.at[5, s])
        wait_bytes(self.full.at[pl.ds(0, 3), pl.ds(0, 14)], self.sends.at[6, s])
        wait_bytes(self.full.at[pl.ds(0, 4), pl.ds(0, 14)], self.sends.at[7, s])


REDUCE_SCRATCH = [
    pltpu.VMEM((2, 4, 14, 16, 128), BF16),
    pltpu.VMEM((2, 4, 14, 16, 128), BF16),
    pltpu.VMEM((2, 3, 14, 16, 128), BF16),
    pltpu.VMEM((2, 16, 16, 128), BF16),
    pltpu.VMEM((2, 3, 4, 16, 128), BF16),
    pltpu.VMEM((2, 8, 8, 128), F32),
    pltpu.VMEM((2, 7, 8, 128), F32),
    pltpu.VMEM((2, 8, 8, 128), F32),
    pltpu.SemaphoreType.DMA((PHASES, 2)),
    pltpu.SemaphoreType.DMA((PHASES, 2)),
]


def enter(place, others):
    barrier = pltpu.get_barrier_semaphore()
    for device in others:
        pl.semaphore_signal(barrier, inc=1, device_id=device, device_id_type=MESH)
    pl.semaphore_wait(barrier, len(others))


def reduce_peers(place):
    peers = [place.twin()]
    peers += [place.peer_x(off)[1] for off in range(1, 4)]
    peers += [place.peer_y(off)[1] for off in range(1, 4)]
    peers += [place.peer_z(off)[1] for off in range(1, 8)]
    return peers


def reduce_kernel(one, two, full_one, full_two, *scratch):
    place = Place()
    enter(place, reduce_peers(place))
    size = len(REDUCE_SCRATCH)
    grads = [
        Reduce(place, two, full_two, *scratch[:size]),
        Reduce(place, one, full_one, *scratch[size:]),
    ]
    todo = [(g, s) for g in grads for s in range(2)]
    for g in grads:
        g.pair_send()
    for g, s in todo:
        g.pair_sum(s)
        g.first_send(s)
    for g, s in todo:
        g.first_sum(s)
        g.second_send(s)
    for g, s in todo:
        g.second_sum(s)
        g.third_send(s)
    for g, s in todo:
        g.third_sum(s)
        g.third_gather(s)
    for g, s in todo:
        g.second_gather(s)
    for g, s in todo:
        g.first_gather(s)
    for g, s in todo:
        g.pair_gather(s)
    for g, s in todo:
        g.finish(s)
    for g, s in todo:
        g.drain(s)


def to_slots(grad):
    tiles = grad.reshape(27, 8, 16, 128).astype(BF16)
    tiles = jnp.swapaxes(tiles, 0, 1)
    hole = jnp.zeros((8, 2, 16, 128), BF16)
    last = jnp.zeros((8, 3, 16, 128), BF16)
    return jnp.concatenate([tiles[:, :14], hole, tiles[:, 14:], last], axis=1)


def from_slots(full, scale):
    tiles = jnp.concatenate([full[:, :14], full[:, 16:29]], axis=1)
    tiles = jnp.swapaxes(tiles, 0, 1).astype(F32) * scale
    return tiles.reshape(3, 3, 3, 128, 128)


def all_sum(one, two, scale):
    shape = jax.ShapeDtypeStruct((8, 32, 16, 128), BF16)
    full_one, full_two = pl.pallas_call(
        reduce_kernel,
        out_shape=(shape, shape),
        in_specs=[pl.BlockSpec(memory_space=pltpu.VMEM)] * 2,
        out_specs=[pl.BlockSpec(memory_space=pltpu.VMEM)] * 2,
        scratch_shapes=REDUCE_SCRATCH + REDUCE_SCRATCH,
        compiler_params=pltpu.CompilerParams(collective_id=0, has_side_effects=True),
    )(to_slots(one), to_slots(two))
    return from_slots(full_one, scale), from_slots(full_two, scale)


def body(volume, cotangent, kernel_one, kernel_two):
    stacked = jnp.stack((volume, cotangent))
    padded_both = padded_2(stacked, (("ta", 1), ("ha", 2), ("wa", 3)), 1)
    volume_pad = padded_both[0]
    cotangent_pad = padded_both[1]
    pre = conv_local(volume_pad, kernel_one)
    sig = jax.nn.sigmoid(pre)
    hidden = (pre * sig).astype(jnp.bfloat16)
    d_hidden = conv_local(cotangent_pad, flip_swap(kernel_two))
    d_pre = (d_hidden * sig * (1.0 + pre * (1.0 - sig))).astype(jnp.bfloat16)
    total_cells = (
        volume.shape[0]
        * volume.shape[1]
        * volume.shape[2]
        * lax.axis_size("ta")
        * lax.axis_size("ha")
        * lax.axis_size("wa")
    )
    scale = 1.0 / jnp.sqrt(jnp.float32(total_cells))
    part_two = flip_swap(kernel_local(cotangent_pad, hidden))
    d_pre_pad = padded_2(d_pre, (("ta", 0), ("ha", 1), ("wa", 2)), 1)
    d_volume = conv_local(d_pre_pad, flip_swap(kernel_one)).astype(jnp.bfloat16)
    part_one = kernel_local(volume_pad, d_pre)
    grad_one, grad_two = all_sum(part_one, part_two, scale)
    return (d_volume, grad_one, grad_two)


def solution(mesh):
    in_specs = (P("ta", "ha", "wa", None), P("ta", "ha", "wa", None), P(), P())
    out_specs = (P("ta", "ha", "wa", None), P(), P())
    return jax.shard_map(body, mesh=mesh, in_specs=in_specs, out_specs=out_specs, check_vma=False)
```

```python
import jax
import jax.numpy as jnp
from jax import lax
from jax.experimental import pallas as pl
from jax.experimental.pallas import tpu as pltpu
from jax.sharding import PartitionSpec as P

MESH = pl.DeviceIdType.MESH
F32 = jnp.float32
BF16 = jnp.bfloat16


class Place:
    def __init__(self):
        self.ta = lax.axis_index("ta")
        self.ha = lax.axis_index("ha")
        self.wa = lax.axis_index("wa")
        self.core = lax.rem(self.wa, 2)
        self.x = lax.rem(self.ta, 4)
        self.y = self.ha
        self.z = (self.wa // 2) * 2 + self.ta // 4

    def peer_x(self, off):
        to = lax.rem(self.x + off, 4)
        return to, (self.ta - self.x + to, self.ha, self.wa)

    def peer_y(self, off):
        to = lax.rem(self.y + off, 4)
        return to, (self.ta, to, self.wa)

    def peer_z(self, off):
        to = lax.rem(self.z + off, 8)
        return to, (lax.rem(to, 2) * 4 + self.x, self.ha, (to // 2) * 2 + self.core)

    def near(self, dta, dha, dwa):
        return (lax.rem(self.ta + dta + 8, 8), lax.rem(self.ha + dha + 4, 4), lax.rem(self.wa + dwa + 8, 8))

    def twin(self):
        return (self.ta, self.ha, self.wa + 1 - 2 * self.core)


def send(src, dst, send_sem, recv_sem, device):
    pltpu.make_async_remote_copy(
        src_ref=src, dst_ref=dst, send_sem=send_sem, recv_sem=recv_sem,
        device_id=device, device_id_type=MESH,
    ).start()


def wait_bytes(ref, sem):
    pltpu.make_async_copy(ref, ref, sem).wait()


PHASES = 8


class Reduce:
    def __init__(self, place, part, full, land0, sums, land1, tops, land2, thirds, land3, lasts, sends, recvs):
        self.at = place
        self.part, self.full = part, full
        self.land0, self.sums, self.land1 = land0, sums, land1
        self.tops, self.land2 = tops, land2
        self.thirds, self.land3, self.lasts = thirds, land3, lasts
        self.sends, self.recvs = sends, recvs

    def first(self, s, off):
        return self.at.peer_x(off) if s == 0 else self.at.peer_y(off)

    def second(self, s, off):
        return self.at.peer_y(off) if s == 0 else self.at.peer_x(off)

    def mine(self, s):
        return (self.at.x, self.at.y) if s == 0 else (self.at.y, self.at.x)

    def pair_send(self):
        other = 4 - 4 * self.at.core
        for s in range(2):
            send(
                self.part.at[pl.ds(other, 4), pl.ds(16 * s, 14)],
                self.land0.at[s],
                self.sends.at[0, s], self.recvs.at[0, s], self.at.twin(),
            )

    def pair_sum(self, s):
        own = 4 * self.at.core
        wait_bytes(self.land0.at[s], self.recvs.at[0, s])

        def step(i, _):
            total = self.part[own + i, pl.ds(16 * s, 14)].astype(F32) + self.land0[s, i].astype(F32)
            self.sums[s, i] = total.astype(BF16)
            return 0

        lax.fori_loop(0, 4, step, 0)

    def first_send(self, s):
        for off in range(1, 4):
            to, device = self.first(s, off)
            send(
                self.sums.at[s, to], self.land1.at[s, off - 1],
                self.sends.at[1, s], self.recvs.at[1, s], device,
            )

    def first_sum(self, s):
        me, _ = self.mine(s)
        wait_bytes(self.land1.at[s], self.recvs.at[1, s])
        total = self.sums[s, me].astype(F32)
        for j in range(3):
            total = total + self.land1[s, j].astype(F32)
        self.tops[s, pl.ds(0, 14)] = total.astype(BF16)
        self.tops[s, pl.ds(14, 2)] = jnp.zeros((2, 16, 128), BF16)

    def second_send(self, s):
        for off in range(1, 4):
            to, device = self.second(s, off)
            send(
                self.tops.at[s, pl.ds(4 * to, 4)], self.land2.at[s, off - 1],
                self.sends.at[2, s], self.recvs.at[2, s], device,
            )

    def second_sum(self, s):
        _, me = self.mine(s)
        wait_bytes(self.land2.at[s], self.recvs.at[2, s])
        total = self.tops[s, pl.ds(4 * me, 4)].astype(F32)
        for j in range(3):
            total = total + self.land2[s, j].astype(F32)
        self.thirds[s] = total.reshape(8, 8, 128)

    def third_send(self, s):
        for off in range(1, 8):
            to, device = self.at.peer_z(off)
            send(
                self.thirds.at[s, to], self.land3.at[s, off - 1],
                self.sends.at[3, s], self.recvs.at[3, s], device,
            )

    def third_sum(self, s):
        wait_bytes(self.land3.at[s], self.recvs.at[3, s])
        total = self.thirds[s, self.at.z]
        for j in range(7):
            total = total + self.land3[s, j]
        self.lasts[s, self.at.z] = total

    def third_gather(self, s):
        for off in range(1, 8):
            _, device = self.at.peer_z(off)
            send(
                self.lasts.at[s, self.at.z], self.lasts.at[s, self.at.z],
                self.sends.at[4, s], self.recvs.at[4, s], device,
            )

    def second_gather(self, s):
        me, me2 = self.mine(s)
        wait_bytes(self.lasts.at[s, pl.ds(0, 7)], self.recvs.at[4, s])
        row = 4 * self.at.core + me
        spot = pl.ds(16 * s + 4 * me2, 4)
        self.full[row, spot] = self.lasts[s].reshape(4, 16, 128).astype(BF16)
        for off in range(1, 4):
            _, device = self.second(s, off)
            send(
                self.full.at[row, spot], self.full.at[row, spot],
                self.sends.at[5, s], self.recvs.at[5, s], device,
            )

    def first_gather(self, s):
        me, me2 = self.mine(s)
        wait_bytes(self.full.at[0, pl.ds(0, 12)], self.recvs.at[5, s])
        row = 4 * self.at.core + me
        spot = pl.ds(16 * s, 14)
        for off in range(1, 4):
            _, device = self.first(s, off)
            send(
                self.full.at[row, spot], self.full.at[row, spot],
                self.sends.at[6, s], self.recvs.at[6, s], device,
            )

    def pair_gather(self, s):
        wait_bytes(self.full.at[pl.ds(0, 3), pl.ds(0, 14)], self.recvs.at[6, s])
        rows = pl.ds(4 * self.at.core, 4)
        spot = pl.ds(16 * s, 14)
        send(
            self.full.at[rows, spot], self.full.at[rows, spot],
            self.sends.at[7, s], self.recvs.at[7, s], self.at.twin(),
        )

    def finish(self, s):
        wait_bytes(self.full.at[pl.ds(0, 4), pl.ds(0, 14)], self.recvs.at[7, s])

    def drain(self, s):
        wait_bytes(self.land0.at[s], self.sends.at[0, s])
        wait_bytes(self.land1.at[s], self.sends.at[1, s])
        wait_bytes(self.land2.at[s], self.sends.at[2, s])
        wait_bytes(self.land3.at[s], self.sends.at[3, s])
        wait_bytes(self.lasts.at[s, pl.ds(0, 7)], self.sends.at[4, s])
        wait_bytes(self.full.at[0, pl.ds(0, 12)], self.sends.at[5, s])
        wait_bytes(self.full.at[pl.ds(0, 3), pl.ds(0, 14)], self.sends.at[6, s])
        wait_bytes(self.full.at[pl.ds(0, 4), pl.ds(0, 14)], self.sends.at[7, s])


REDUCE_SCRATCH = [
    pltpu.VMEM((2, 4, 14, 16, 128), BF16),
    pltpu.VMEM((2, 4, 14, 16, 128), BF16),
    pltpu.VMEM((2, 3, 14, 16, 128), BF16),
    pltpu.VMEM((2, 16, 16, 128), BF16),
    pltpu.VMEM((2, 3, 4, 16, 128), BF16),
    pltpu.VMEM((2, 8, 8, 128), F32),
    pltpu.VMEM((2, 7, 8, 128), F32),
    pltpu.VMEM((2, 8, 8, 128), F32),
    pltpu.SemaphoreType.DMA((PHASES, 2)),
    pltpu.SemaphoreType.DMA((PHASES, 2)),
]


def reduce_peers(place):
    peers = [place.twin()]
    peers += [place.peer_x(off)[1] for off in range(1, 4)]
    peers += [place.peer_y(off)[1] for off in range(1, 4)]
    peers += [place.peer_z(off)[1] for off in range(1, 8)]
    return peers


class Field:
    def __init__(self, place, raw, wide, cols, ends, cols_out, ends_out, win, sends, recvs):
        self.at = place
        self.raw, self.wide = raw, wide
        self.cols, self.ends, self.cols_out, self.ends_out = cols, ends, cols_out, ends_out
        self.win, self.sends, self.recvs = win, sends, recvs

    def stage(self):
        own = self.raw[1, pl.ds(1, 32)].astype(F32)
        self.wide[...] = own.reshape(512, 128)
        self.cols_out[0] = self.wide[pl.ds(0, 32, stride=16), :].astype(BF16)
        self.cols_out[1] = self.wide[pl.ds(15, 32, stride=16), :].astype(BF16)
        self.ends_out[0] = self.wide[pl.ds(0, 1), :]
        self.ends_out[1] = self.wide[pl.ds(496, 1), :]
        self.ends_out[2] = self.wide[pl.ds(15, 1), :]
        self.ends_out[3] = self.wide[pl.ds(511, 1), :]

    def go(self, kind, src, dst, device):
        send(src, dst, self.sends.at[kind], self.recvs.at[kind], device)

    def frame_send(self):
        near = self.at.near
        self.go(0, self.raw.at[1, 1], self.raw.at[1, 33], near(0, -1, 0))
        self.go(0, self.raw.at[1, 32], self.raw.at[1, 0], near(0, 1, 0))
        self.go(1, self.cols_out.at[0], self.cols.at[1, 1], near(0, 0, -1))
        self.go(1, self.cols_out.at[1], self.cols.at[1, 0], near(0, 0, 1))
        self.go(2, self.ends_out.at[0], self.ends.at[1, 3], near(0, -1, -1))
        self.go(2, self.ends_out.at[1], self.ends.at[1, 2], near(0, 1, -1))
        self.go(2, self.ends_out.at[2], self.ends.at[1, 1], near(0, -1, 1))
        self.go(2, self.ends_out.at[3], self.ends.at[1, 0], near(0, 1, 1))

    def bulk_send(self):
        near = self.at.near
        own = self.raw.at[1, pl.ds(1, 32)]
        self.go(3, own, self.raw.at[0, pl.ds(1, 32)], near(1, 0, 0))
        self.go(3, own, self.raw.at[2, pl.ds(1, 32)], near(-1, 0, 0))

    def frame_wait(self):
        wait_bytes(self.raw.at[1, pl.ds(0, 2)], self.recvs.at[0])
        wait_bytes(self.cols.at[1], self.recvs.at[1])
        wait_bytes(self.ends.at[1], self.recvs.at[2])

    def rim_send(self):
        for frame, step in ((0, 1), (2, -1)):
            device = self.at.near(step, 0, 0)
            self.go(4, self.raw.at[1, 0], self.raw.at[frame, 0], device)
            self.go(4, self.raw.at[1, 33], self.raw.at[frame, 33], device)
            self.go(5, self.cols.at[1], self.cols.at[frame], device)
            self.go(6, self.ends.at[1], self.ends.at[frame], device)

    def times_wait(self):
        wait_bytes(self.raw.at[pl.ds(0, 2), pl.ds(0, 32)], self.recvs.at[3])
        wait_bytes(self.raw.at[0, pl.ds(0, 4)], self.recvs.at[4])
        wait_bytes(self.cols.at[pl.ds(0, 2)], self.recvs.at[5])
        wait_bytes(self.ends.at[pl.ds(0, 2)], self.recvs.at[6])

    def drain(self):
        wait_bytes(self.raw.at[1, pl.ds(0, 2)], self.sends.at[0])
        wait_bytes(self.cols.at[1], self.sends.at[1])
        wait_bytes(self.ends.at[1], self.sends.at[2])
        wait_bytes(self.raw.at[pl.ds(0, 2), pl.ds(0, 32)], self.sends.at[3])
        wait_bytes(self.raw.at[0, pl.ds(0, 4)], self.sends.at[4])
        wait_bytes(self.cols.at[pl.ds(0, 2)], self.sends.at[5])
        wait_bytes(self.ends.at[pl.ds(0, 2)], self.sends.at[6])

    def windows(self, frame):
        spot = lax.broadcasted_iota(jnp.int32, (16, 128), 0)
        at_left, at_right = self.at.wa == 0, self.at.wa == 7

        def line(row, left, right):
            mid = self.raw[frame, row]
            wide = mid.astype(F32)
            left = jnp.where(at_left, 0.0, left)
            right = jnp.where(at_right, 0.0, right)
            before = jnp.where(spot == 0, left, pltpu.roll(wide, 1, 0))
            after = jnp.where(spot == 15, right, pltpu.roll(wide, 15, 0))
            self.win[frame, row, :, pl.ds(0, 128)] = before.astype(BF16)
            self.win[frame, row, :, pl.ds(128, 128)] = mid
            self.win[frame, row, :, pl.ds(256, 128)] = after.astype(BF16)

        def group(g, _):
            start = pl.multiple_of(16 * g, 16)
            left = self.cols[frame, 0, pl.ds(start, 16), :].astype(F32)
            right = self.cols[frame, 1, pl.ds(start, 16), :].astype(F32)
            for r in range(16):
                line(16 * g + r + 1, left[r : r + 1], right[r : r + 1])
            return 0

        lax.fori_loop(0, 2, group, 0)
        line(0, self.ends[frame, 0], self.ends[frame, 2])
        line(33, self.ends[frame, 1], self.ends[frame, 3])
        blank = jnp.zeros((16, 384), BF16)

        @pl.when(self.at.ha == 0)
        def _():
            self.win[frame, 0] = blank

        @pl.when(self.at.ha == 3)
        def _():
            self.win[frame, 33] = blank

        if frame != 1:

            @pl.when(self.at.ta == (0 if frame == 0 else 7))
            def _():
                self.win[frame] = jnp.zeros((34, 16, 384), BF16)

    def taps(self, weights, frame):
        rows = [weights[pl.ds(9 * frame + 3 * kh, 3)].reshape(384, 128) for kh in range(3)]
        return jnp.concatenate(rows, axis=1)

    def middle(self, weights, out):
        lhs = self.win[1].reshape(544, 384)
        out[...] = jnp.dot(lhs, self.taps(weights, 1), preferred_element_type=F32).reshape(34, 16, 384)

    def outer(self, weights, out):
        lhs = jnp.concatenate([self.win[0].reshape(544, 384), self.win[2].reshape(544, 384)], axis=1)
        rhs = jnp.concatenate([self.taps(weights, 0), self.taps(weights, 2)], axis=0)
        out[...] = out[...] + jnp.dot(lhs, rhs, preferred_element_type=F32).reshape(34, 16, 384)


FIELD_SCRATCH = [
    pltpu.VMEM((3, 34, 16, 128), BF16),
    pltpu.VMEM((512, 128), F32),
    pltpu.VMEM((3, 2, 32, 128), BF16),
    pltpu.VMEM((3, 4, 1, 128), F32),
    pltpu.VMEM((2, 32, 128), BF16),
    pltpu.VMEM((4, 1, 128), F32),
    pltpu.VMEM((3, 34, 16, 384), BF16),
    pltpu.SemaphoreType.DMA((7,)),
    pltpu.SemaphoreType.DMA((7,)),
]


def shifted(out, row):
    return (
        out[pl.ds(row, 4), :, pl.ds(0, 128)]
        + out[pl.ds(row + 1, 4), :, pl.ds(128, 128)]
        + out[pl.ds(row + 2, 4), :, pl.ds(256, 128)]
    )


def slot_of(tap):
    return tap if tap < 14 else tap + 2


def transposed(weights, out):
    def step(n, _):
        out[n] = weights[26 - n].T
        return 0

    lax.fori_loop(0, 27, step, 0)


def block_kernel(vol_hbm, cot_hbm, one_hbm, two_hbm, d_vol, full_one, full_two, *scratch):
    place = Place()
    barrier = pltpu.get_barrier_semaphore()
    others = reduce_peers(place)
    others += [place.near(s, 0, 0) for s in (1, -1)]
    others += [place.near(0, 0, s) for s in (1, -1)]
    others += [place.near(0, a, b) for a in (1, -1) for b in (1, -1)]
    for device in others:
        pl.semaphore_signal(barrier, inc=1, device_id=device, device_id_type=MESH)

    f, r = len(FIELD_SCRATCH), len(REDUCE_SCRATCH)
    vol = Field(place, *scratch[:f])
    cot = Field(place, *scratch[f : 2 * f])
    dpre = Field(place, *scratch[2 * f : 3 * f])
    scratch = scratch[3 * f :]
    part_one, part_two = scratch[0], scratch[1]
    red_two = Reduce(place, part_two, full_two, *scratch[2 : 2 + r])
    red_one = Reduce(place, part_one, full_one, *scratch[2 + r : 2 + 2 * r])
    scratch = scratch[2 + 2 * r :]
    one, two, one_t, two_t, out_v, out_c, gate, act, act_t, local = scratch

    loads = [
        pltpu.make_async_copy(vol_hbm, vol.raw.at[1, pl.ds(1, 32)], local.at[0]),
        pltpu.make_async_copy(cot_hbm, cot.raw.at[1, pl.ds(1, 32)], local.at[1]),
        pltpu.make_async_copy(two_hbm, two, local.at[2]),
        pltpu.make_async_copy(one_hbm, one, local.at[3]),
    ]
    for load in loads:
        load.start()
    part_one[:, 29] = jnp.zeros((8, 16, 128), BF16)
    part_two[:, 29] = jnp.zeros((8, 16, 128), BF16)
    loads[0].wait()
    vol.stage()
    loads[1].wait()
    cot.stage()
    pl.semaphore_wait(barrier, len(others))

    vol.bulk_send()
    vol.frame_send()
    cot.frame_send()
    loads[2].wait()
    transposed(two, two_t)
    loads[3].wait()
    vol.frame_wait()
    vol.rim_send()
    cot.bulk_send()
    vol.windows(1)
    cot.frame_wait()
    cot.rim_send()
    cot.windows(1)
    vol.middle(one, out_v)
    cot.middle(two_t, out_c)
    transposed(one, one_t)

    vol.times_wait()
    vol.windows(0)
    vol.windows(2)
    vol.outer(one, out_v)

    def activate(g, _):
        row = 4 * g
        pre = shifted(out_v, row)
        sig = 1.0 / (1.0 + jnp.exp(-pre))
        act[pl.ds(row, 4)] = (pre * sig).astype(BF16)
        gate[pl.ds(row, 4)] = sig * (1.0 + pre * (1.0 - sig))
        return 0

    lax.fori_loop(0, 8, activate, 0)
    act_t[...] = act[...].reshape(512, 128).T

    cot.times_wait()
    cot.windows(0)
    cot.windows(2)
    for t in range(3):
        for kh in range(3):
            rhs = cot.win[t, pl.ds(kh, 32)].reshape(512, 384)
            got = jnp.dot(act_t[...], rhs, preferred_element_type=F32)
            for kw in range(3):
                tap = 26 - (9 * t + 3 * kh + kw)
                block = got[:, 128 * kw : 128 * kw + 128].reshape(8, 16, 128)
                part_two[:, slot_of(tap)] = block.astype(BF16)
    red_two.pair_send()

    cot.outer(two_t, out_c)

    def backward(g, _):
        row = 4 * g
        dpre.raw[1, pl.ds(row + 1, 4)] = (shifted(out_c, row) * gate[pl.ds(row, 4)]).astype(BF16)
        return 0

    lax.fori_loop(0, 8, backward, 0)
    dpre.stage()
    dpre.frame_send()
    act_t[...] = dpre.raw[1, pl.ds(1, 32)].reshape(512, 128).T
    for s in range(2):
        red_two.pair_sum(s)
        red_two.first_send(s)
    for t in range(3):
        for kh in range(3):
            rhs = vol.win[t, pl.ds(kh, 32)].reshape(512, 384)
            got = jnp.dot(act_t[...], rhs, preferred_element_type=F32)
            for kw in range(3):
                tap = 9 * t + 3 * kh + kw
                block = got[:, 128 * kw : 128 * kw + 128].T.reshape(8, 16, 128)
                part_one[:, slot_of(tap)] = block.astype(BF16)
    red_one.pair_send()
    for s in range(2):
        red_two.first_sum(s)
        red_two.second_send(s)
    for s in range(2):
        red_one.pair_sum(s)
        red_one.first_send(s)
    dpre.frame_wait()
    dpre.bulk_send()
    dpre.rim_send()
    dpre.windows(1)
    for s in range(2):
        red_two.second_sum(s)
        red_two.third_send(s)
    dpre.middle(one_t, out_v)
    for s in range(2):
        red_one.first_sum(s)
        red_one.second_send(s)
    for s in range(2):
        red_two.third_sum(s)
        red_two.third_gather(s)
    for s in range(2):
        red_one.second_sum(s)
        red_one.third_send(s)
    dpre.times_wait()
    dpre.windows(0)
    dpre.windows(2)
    dpre.outer(one_t, out_v)

    def finish(g, _):
        row = 4 * g
        d_vol[pl.ds(row, 4)] = shifted(out_v, row).astype(BF16)
        return 0

    lax.fori_loop(0, 8, finish, 0)
    for s in range(2):
        red_two.second_gather(s)
    for s in range(2):
        red_one.third_sum(s)
        red_one.third_gather(s)
    for s in range(2):
        red_two.first_gather(s)
    for s in range(2):
        red_one.second_gather(s)
    for s in range(2):
        red_two.pair_gather(s)
    for s in range(2):
        red_one.first_gather(s)
    for s in range(2):
        red_one.pair_gather(s)
    for red in (red_two, red_one):
        for s in range(2):
            red.finish(s)
            red.drain(s)
    for field in (vol, cot, dpre):
        field.drain()


def from_slots(full, scale):
    tiles = jnp.concatenate([full[:, :14], full[:, 16:29]], axis=1)
    tiles = jnp.swapaxes(tiles, 0, 1).astype(F32) * scale
    return tiles.reshape(3, 3, 3, 128, 128)


def body(volume, cotangent, kernel_one, kernel_two):
    total_cells = (
        volume.shape[0]
        * volume.shape[1]
        * volume.shape[2]
        * lax.axis_size("ta")
        * lax.axis_size("ha")
        * lax.axis_size("wa")
    )
    scale = 1.0 / jnp.sqrt(jnp.float32(total_cells))
    full = jax.ShapeDtypeStruct((8, 32, 16, 128), BF16)
    taps = pltpu.VMEM((27, 128, 128), BF16)
    d_volume, full_one, full_two = pl.pallas_call(
        block_kernel,
        out_shape=(jax.ShapeDtypeStruct((32, 16, 128), BF16), full, full),
        in_specs=[pl.BlockSpec(memory_space=pl.ANY)] * 4,
        out_specs=[pl.BlockSpec(memory_space=pltpu.VMEM)] * 3,
        scratch_shapes=FIELD_SCRATCH * 3
        + [pltpu.VMEM((8, 32, 16, 128), BF16)] * 2
        + REDUCE_SCRATCH * 2
        + [taps] * 4
        + [pltpu.VMEM((34, 16, 384), F32)] * 2
        + [
            pltpu.VMEM((32, 16, 128), F32),
            pltpu.VMEM((32, 16, 128), BF16),
            pltpu.VMEM((128, 512), BF16),
            pltpu.SemaphoreType.DMA((4,)),
        ],
        compiler_params=pltpu.CompilerParams(
            collective_id=0, has_side_effects=True, vmem_limit_bytes=60 * 1024 * 1024
        ),
    )(
        volume.reshape(32, 16, 128),
        cotangent.reshape(32, 16, 128),
        kernel_one.reshape(27, 128, 128),
        kernel_two.reshape(27, 128, 128),
    )
    return (
        d_volume.reshape(volume.shape),
        from_slots(full_one, scale),
        from_slots(full_two, scale),
    )


def solution(mesh):
    in_specs = (P("ta", "ha", "wa", None), P("ta", "ha", "wa", None), P(), P())
    out_specs = (P("ta", "ha", "wa", None), P(), P())
    return jax.shard_map(body, mesh=mesh, in_specs=in_specs, out_specs=out_specs, check_vma=False)
```

```python
import functools

import jax
import jax.numpy as jnp
import numpy as np
from jax import lax
from jax.experimental import pallas as pl
from jax.experimental.pallas import tpu as pltpu
from jax.sharding import PartitionSpec as P

MESH = pl.DeviceIdType.MESH
F32 = jnp.float32
BF16 = jnp.bfloat16


class Place:
    def __init__(self):
        self.ta = lax.axis_index("ta")
        self.ha = lax.axis_index("ha")
        self.wa = lax.axis_index("wa")
        self.core = lax.rem(self.wa, 2)
        self.x = lax.rem(self.ta, 4)
        self.y = self.ha
        self.z = (self.wa // 2) * 2 + self.ta // 4

    def peer_x(self, off):
        to = lax.rem(self.x + off, 4)
        return to, (self.ta - self.x + to, self.ha, self.wa)

    def peer_y(self, off):
        to = lax.rem(self.y + off, 4)
        return to, (self.ta, to, self.wa)

    def peer_z(self, off):
        to = lax.rem(self.z + off, 8)
        return to, (lax.rem(to, 2) * 4 + self.x, self.ha, (to // 2) * 2 + self.core)

    def near(self, dta, dha, dwa):
        return (lax.rem(self.ta + dta + 8, 8), lax.rem(self.ha + dha + 4, 4), lax.rem(self.wa + dwa + 8, 8))

    def twin(self):
        return (self.ta, self.ha, self.wa + 1 - 2 * self.core)


def send(src, dst, send_sem, recv_sem, device):
    pltpu.make_async_remote_copy(
        src_ref=src, dst_ref=dst, send_sem=send_sem, recv_sem=recv_sem,
        device_id=device, device_id_type=MESH,
    ).start()


def wait_bytes(ref, sem):
    pltpu.make_async_copy(ref, ref, sem).wait()


PHASES = 8


class Reduce:
    def __init__(self, place, part, full, land0, sums, land1, tops, land2, thirds, land3, lasts, sends, recvs):
        self.at = place
        self.part, self.full = part, full
        self.land0, self.sums, self.land1 = land0, sums, land1
        self.tops, self.land2 = tops, land2
        self.thirds, self.land3, self.lasts = thirds, land3, lasts
        self.sends, self.recvs = sends, recvs

    def first(self, s, off):
        return self.at.peer_x(off) if s == 0 else self.at.peer_y(off)

    def second(self, s, off):
        return self.at.peer_y(off) if s == 0 else self.at.peer_x(off)

    def mine(self, s):
        return (self.at.x, self.at.y) if s == 0 else (self.at.y, self.at.x)

    def pair_send(self):
        other = 4 - 4 * self.at.core
        for s in range(2):
            send(
                self.part.at[pl.ds(other, 4), pl.ds(16 * s, 14)],
                self.land0.at[s],
                self.sends.at[0, s], self.recvs.at[0, s], self.at.twin(),
            )

    def pair_sum(self, s):
        own = 4 * self.at.core
        wait_bytes(self.land0.at[s], self.recvs.at[0, s])

        def step(i, _):
            total = self.part[own + i, pl.ds(16 * s, 14)].astype(F32) + self.land0[s, i].astype(F32)
            self.sums[s, i] = total.astype(BF16)
            return 0

        lax.fori_loop(0, 4, step, 0)

    def first_send(self, s):
        for off in range(1, 4):
            to, device = self.first(s, off)
            send(
                self.sums.at[s, to], self.land1.at[s, off - 1],
                self.sends.at[1, s], self.recvs.at[1, s], device,
            )

    def first_sum(self, s):
        me, _ = self.mine(s)
        wait_bytes(self.land1.at[s], self.recvs.at[1, s])
        total = self.sums[s, me].astype(F32)
        for j in range(3):
            total = total + self.land1[s, j].astype(F32)
        self.tops[s, pl.ds(0, 14)] = total.astype(BF16)
        self.tops[s, pl.ds(14, 2)] = jnp.zeros((2, 16, 128), BF16)

    def second_send(self, s):
        for off in range(1, 4):
            to, device = self.second(s, off)
            send(
                self.tops.at[s, pl.ds(4 * to, 4)], self.land2.at[s, off - 1],
                self.sends.at[2, s], self.recvs.at[2, s], device,
            )

    def second_sum(self, s):
        _, me = self.mine(s)
        wait_bytes(self.land2.at[s], self.recvs.at[2, s])
        total = self.tops[s, pl.ds(4 * me, 4)].astype(F32)
        for j in range(3):
            total = total + self.land2[s, j].astype(F32)
        self.thirds[s] = total.reshape(8, 8, 128)

    def third_send(self, s):
        for off in range(1, 8):
            to, device = self.at.peer_z(off)
            send(
                self.thirds.at[s, to], self.land3.at[s, off - 1],
                self.sends.at[3, s], self.recvs.at[3, s], device,
            )

    def third_sum(self, s):
        wait_bytes(self.land3.at[s], self.recvs.at[3, s])
        total = self.thirds[s, self.at.z]
        for j in range(7):
            total = total + self.land3[s, j]
        self.lasts[s, self.at.z] = total

    def third_gather(self, s):
        for off in range(1, 8):
            _, device = self.at.peer_z(off)
            send(
                self.lasts.at[s, self.at.z], self.lasts.at[s, self.at.z],
                self.sends.at[4, s], self.recvs.at[4, s], device,
            )

    def second_gather(self, s):
        me, me2 = self.mine(s)
        wait_bytes(self.lasts.at[s, pl.ds(0, 7)], self.recvs.at[4, s])
        row = 4 * self.at.core + me
        spot = pl.ds(16 * s + 4 * me2, 4)
        self.full[row, spot] = self.lasts[s].reshape(4, 16, 128).astype(BF16)
        for off in range(1, 4):
            _, device = self.second(s, off)
            send(
                self.full.at[row, spot], self.full.at[row, spot],
                self.sends.at[5, s], self.recvs.at[5, s], device,
            )

    def first_gather(self, s):
        me, me2 = self.mine(s)
        wait_bytes(self.full.at[0, pl.ds(0, 12)], self.recvs.at[5, s])
        row = 4 * self.at.core + me
        spot = pl.ds(16 * s, 14)
        for off in range(1, 4):
            _, device = self.first(s, off)
            send(
                self.full.at[row, spot], self.full.at[row, spot],
                self.sends.at[6, s], self.recvs.at[6, s], device,
            )

    def pair_gather(self, s):
        wait_bytes(self.full.at[pl.ds(0, 3), pl.ds(0, 14)], self.recvs.at[6, s])
        rows = pl.ds(4 * self.at.core, 4)
        spot = pl.ds(16 * s, 14)
        send(
            self.full.at[rows, spot], self.full.at[rows, spot],
            self.sends.at[7, s], self.recvs.at[7, s], self.at.twin(),
        )

    def finish(self, s):
        wait_bytes(self.full.at[pl.ds(0, 4), pl.ds(0, 14)], self.recvs.at[7, s])

    def drain(self, s):
        wait_bytes(self.land0.at[s], self.sends.at[0, s])
        wait_bytes(self.land1.at[s], self.sends.at[1, s])
        wait_bytes(self.land2.at[s], self.sends.at[2, s])
        wait_bytes(self.land3.at[s], self.sends.at[3, s])
        wait_bytes(self.lasts.at[s, pl.ds(0, 7)], self.sends.at[4, s])
        wait_bytes(self.full.at[0, pl.ds(0, 12)], self.sends.at[5, s])
        wait_bytes(self.full.at[pl.ds(0, 3), pl.ds(0, 14)], self.sends.at[6, s])
        wait_bytes(self.full.at[pl.ds(0, 4), pl.ds(0, 14)], self.sends.at[7, s])


REDUCE_SCRATCH = [
    pltpu.VMEM((2, 4, 14, 16, 128), BF16),
    pltpu.VMEM((2, 4, 14, 16, 128), BF16),
    pltpu.VMEM((2, 3, 14, 16, 128), BF16),
    pltpu.VMEM((2, 16, 16, 128), BF16),
    pltpu.VMEM((2, 3, 4, 16, 128), BF16),
    pltpu.VMEM((2, 8, 8, 128), F32),
    pltpu.VMEM((2, 7, 8, 128), F32),
    pltpu.VMEM((2, 8, 8, 128), F32),
    pltpu.SemaphoreType.DMA((PHASES, 2)),
    pltpu.SemaphoreType.DMA((PHASES, 2)),
]


def reduce_peers(place):
    peers = [place.twin()]
    peers += [place.peer_x(off)[1] for off in range(1, 4)]
    peers += [place.peer_y(off)[1] for off in range(1, 4)]
    peers += [place.peer_z(off)[1] for off in range(1, 8)]
    return peers


class Field:
    def __init__(self, place, raw, wide, cols, ends, cols_out, ends_out, win, sends, recvs):
        self.at = place
        self.raw, self.wide = raw, wide
        self.cols, self.ends, self.cols_out, self.ends_out = cols, ends, cols_out, ends_out
        self.win, self.sends, self.recvs = win, sends, recvs

    def stage(self):
        own = self.raw[1, pl.ds(1, 32)].astype(F32)
        self.wide[...] = own.reshape(512, 128)
        self.cols_out[0] = self.wide[pl.ds(0, 32, stride=16), :].astype(BF16)
        self.cols_out[1] = self.wide[pl.ds(15, 32, stride=16), :].astype(BF16)
        self.ends_out[0] = self.wide[pl.ds(0, 1), :]
        self.ends_out[1] = self.wide[pl.ds(496, 1), :]
        self.ends_out[2] = self.wide[pl.ds(15, 1), :]
        self.ends_out[3] = self.wide[pl.ds(511, 1), :]

    def go(self, kind, src, dst, device):
        send(src, dst, self.sends.at[kind], self.recvs.at[kind], device)

    def frame_send(self):
        near = self.at.near
        self.go(0, self.raw.at[1, 1], self.raw.at[1, 33], near(0, -1, 0))
        self.go(0, self.raw.at[1, 32], self.raw.at[1, 0], near(0, 1, 0))
        self.go(1, self.cols_out.at[0], self.cols.at[1, 1], near(0, 0, -1))
        self.go(1, self.cols_out.at[1], self.cols.at[1, 0], near(0, 0, 1))
        self.go(2, self.ends_out.at[0], self.ends.at[1, 3], near(0, -1, -1))
        self.go(2, self.ends_out.at[1], self.ends.at[1, 2], near(0, 1, -1))
        self.go(2, self.ends_out.at[2], self.ends.at[1, 1], near(0, -1, 1))
        self.go(2, self.ends_out.at[3], self.ends.at[1, 0], near(0, 1, 1))

    def bulk_send(self, half):
        near = self.at.near
        rows = pl.ds(1 + 16 * half, 16)
        own = self.raw.at[1, rows]
        self.go(3, own, self.raw.at[0, rows], near(1, 0, 0))
        self.go(3, own, self.raw.at[2, rows], near(-1, 0, 0))

    def frame_wait(self):
        wait_bytes(self.raw.at[1, pl.ds(0, 2)], self.recvs.at[0])
        wait_bytes(self.cols.at[1], self.recvs.at[1])
        wait_bytes(self.ends.at[1], self.recvs.at[2])

    def rim_send(self):
        for frame, step in ((0, 1), (2, -1)):
            device = self.at.near(step, 0, 0)
            self.go(4, self.raw.at[1, 0], self.raw.at[frame, 0], device)
            self.go(4, self.raw.at[1, 33], self.raw.at[frame, 33], device)
            self.go(5, self.cols.at[1], self.cols.at[frame], device)
            self.go(6, self.ends.at[1], self.ends.at[frame], device)

    def times_wait(self):
        wait_bytes(self.raw.at[pl.ds(0, 2), pl.ds(0, 32)], self.recvs.at[3])
        wait_bytes(self.raw.at[0, pl.ds(0, 4)], self.recvs.at[4])
        wait_bytes(self.cols.at[pl.ds(0, 2)], self.recvs.at[5])
        wait_bytes(self.ends.at[pl.ds(0, 2)], self.recvs.at[6])

    def drain(self):
        wait_bytes(self.raw.at[1, pl.ds(0, 2)], self.sends.at[0])
        wait_bytes(self.cols.at[1], self.sends.at[1])
        wait_bytes(self.ends.at[1], self.sends.at[2])
        wait_bytes(self.raw.at[pl.ds(0, 2), pl.ds(0, 32)], self.sends.at[3])
        wait_bytes(self.raw.at[0, pl.ds(0, 4)], self.sends.at[4])
        wait_bytes(self.cols.at[pl.ds(0, 2)], self.sends.at[5])
        wait_bytes(self.ends.at[pl.ds(0, 2)], self.sends.at[6])

    def windows(self, frame):
        spot = lax.broadcasted_iota(jnp.int32, (16, 128), 0)
        at_left, at_right = self.at.wa == 0, self.at.wa == 7

        def line(row, left, right):
            mid = self.raw[frame, row]
            wide = mid.astype(F32)
            left = jnp.where(at_left, 0.0, left)
            right = jnp.where(at_right, 0.0, right)
            before = jnp.where(spot == 0, left, pltpu.roll(wide, 1, 0))
            after = jnp.where(spot == 15, right, pltpu.roll(wide, 15, 0))
            self.win[frame, row, :, pl.ds(0, 128)] = before.astype(BF16)
            self.win[frame, row, :, pl.ds(128, 128)] = mid
            self.win[frame, row, :, pl.ds(256, 128)] = after.astype(BF16)

        def group(g, _):
            start = pl.multiple_of(16 * g, 16)
            left = self.cols[frame, 0, pl.ds(start, 16), :].astype(F32)
            right = self.cols[frame, 1, pl.ds(start, 16), :].astype(F32)
            for r in range(16):
                line(16 * g + r + 1, left[r : r + 1], right[r : r + 1])
            return 0

        lax.fori_loop(0, 2, group, 0)
        line(0, self.ends[frame, 0], self.ends[frame, 2])
        line(33, self.ends[frame, 1], self.ends[frame, 3])
        blank = jnp.zeros((16, 384), BF16)

        @pl.when(self.at.ha == 0)
        def _():
            self.win[frame, 0] = blank

        @pl.when(self.at.ha == 3)
        def _():
            self.win[frame, 33] = blank

        if frame != 1:

            @pl.when(self.at.ta == (0 if frame == 0 else 7))
            def _():
                self.win[frame] = jnp.zeros((34, 16, 384), BF16)

    def taps(self, weights, frame):
        rows = [weights[pl.ds(9 * frame + 3 * kh, 3)].reshape(384, 128) for kh in range(3)]
        return jnp.concatenate(rows, axis=1)

    def middle(self, weights, out):
        lhs = self.win[1].reshape(544, 384)
        out[...] = jnp.dot(lhs, self.taps(weights, 1), preferred_element_type=F32).reshape(34, 16, 384)

    def outer(self, weights, out):
        lhs = jnp.concatenate([self.win[0].reshape(544, 384), self.win[2].reshape(544, 384)], axis=1)
        rhs = jnp.concatenate([self.taps(weights, 0), self.taps(weights, 2)], axis=0)
        out[...] = out[...] + jnp.dot(lhs, rhs, preferred_element_type=F32).reshape(34, 16, 384)


FIELD_SCRATCH = [
    pltpu.VMEM((3, 34, 16, 128), BF16),
    pltpu.VMEM((512, 128), F32),
    pltpu.VMEM((3, 2, 32, 128), BF16),
    pltpu.VMEM((3, 4, 1, 128), F32),
    pltpu.VMEM((2, 32, 128), BF16),
    pltpu.VMEM((4, 1, 128), F32),
    pltpu.VMEM((3, 34, 16, 384), BF16),
    pltpu.SemaphoreType.DMA((7,)),
    pltpu.SemaphoreType.DMA((7,)),
]


def shifted(out, row):
    return (
        out[pl.ds(row, 4), :, pl.ds(0, 128)]
        + out[pl.ds(row + 1, 4), :, pl.ds(128, 128)]
        + out[pl.ds(row + 2, 4), :, pl.ds(256, 128)]
    )


def slot_of(tap):
    return tap if tap < 14 else tap + 2


def transposed(weights, out):
    def step(n, _):
        out[n] = weights[26 - n].T
        return 0

    lax.fori_loop(0, 27, step, 0)


def block_kernel(vol_hbm, cot_hbm, one_hbm, two_hbm, d_vol, full_one, full_two, *scratch):
    place = Place()
    barrier = pltpu.get_barrier_semaphore()
    others = reduce_peers(place)
    others += [place.near(s, 0, 0) for s in (1, -1)]
    others += [place.near(0, 0, s) for s in (1, -1)]
    others += [place.near(0, a, b) for a in (1, -1) for b in (1, -1)]
    for device in others:
        pl.semaphore_signal(barrier, inc=1, device_id=device, device_id_type=MESH)

    f, r = len(FIELD_SCRATCH), len(REDUCE_SCRATCH)
    vol = Field(place, *scratch[:f])
    cot = Field(place, *scratch[f : 2 * f])
    dpre = Field(place, *scratch[2 * f : 3 * f])
    scratch = scratch[3 * f :]
    part_one, part_two = scratch[0], scratch[1]
    red_two = Reduce(place, part_two, full_two, *scratch[2 : 2 + r])
    red_one = Reduce(place, part_one, full_one, *scratch[2 + r : 2 + 2 * r])
    scratch = scratch[2 + 2 * r :]
    one, two, one_t, two_t, out_v, out_c, gate, act, act_t, local = scratch

    loads = [
        pltpu.make_async_copy(vol_hbm, vol.raw.at[1, pl.ds(1, 32)], local.at[0]),
        pltpu.make_async_copy(cot_hbm, cot.raw.at[1, pl.ds(1, 32)], local.at[1]),
        pltpu.make_async_copy(two_hbm, two, local.at[2]),
        pltpu.make_async_copy(one_hbm, one, local.at[3]),
    ]
    for load in loads:
        load.start()
    part_one[:, 29] = jnp.zeros((8, 16, 128), BF16)
    part_two[:, 29] = jnp.zeros((8, 16, 128), BF16)
    loads[0].wait()
    vol.stage()
    loads[1].wait()
    cot.stage()
    pl.semaphore_wait(barrier, len(others))

    vol.frame_send()
    vol.bulk_send(0)
    vol.bulk_send(1)
    cot.frame_send()
    cot.bulk_send(0)
    loads[2].wait()
    transposed(two, two_t)
    loads[3].wait()
    vol.frame_wait()
    vol.rim_send()
    cot.bulk_send(1)
    cot.frame_wait()
    cot.rim_send()
    vol.windows(1)
    cot.windows(1)
    vol.middle(one, out_v)
    cot.middle(two_t, out_c)

    vol.times_wait()
    vol.windows(0)
    vol.windows(2)
    vol.outer(one, out_v)

    def activate(g, _):
        row = 4 * g
        pre = shifted(out_v, row)
        sig = 1.0 / (1.0 + jnp.exp(-pre))
        act[pl.ds(row, 4)] = (pre * sig).astype(BF16)
        gate[pl.ds(row, 4)] = sig * (1.0 + pre * (1.0 - sig))
        return 0

    lax.fori_loop(0, 8, activate, 0)
    act_t[...] = act[...].reshape(512, 128).T

    cot.times_wait()
    cot.windows(0)
    cot.windows(2)
    for t in range(3):
        for kh in range(3):
            rhs = cot.win[t, pl.ds(kh, 32)].reshape(512, 384)
            got = jnp.dot(act_t[...], rhs, preferred_element_type=F32)
            for kw in range(3):
                tap = 26 - (9 * t + 3 * kh + kw)
                block = got[:, 128 * kw : 128 * kw + 128].reshape(8, 16, 128)
                part_two[:, slot_of(tap)] = block.astype(BF16)
    red_two.pair_send()

    cot.outer(two_t, out_c)

    def backward(g, _):
        row = 4 * g
        dpre.raw[1, pl.ds(row + 1, 4)] = (shifted(out_c, row) * gate[pl.ds(row, 4)]).astype(BF16)
        return 0

    lax.fori_loop(0, 8, backward, 0)
    dpre.stage()
    dpre.frame_send()
    act_t[...] = dpre.raw[1, pl.ds(1, 32)].reshape(512, 128).T
    for t in range(3):
        for kh in range(3):
            rhs = vol.win[t, pl.ds(kh, 32)].reshape(512, 384)
            got = jnp.dot(act_t[...], rhs, preferred_element_type=F32)
            for kw in range(3):
                tap = 9 * t + 3 * kh + kw
                block = got[:, 128 * kw : 128 * kw + 128].T.reshape(8, 16, 128)
                part_one[:, slot_of(tap)] = block.astype(BF16)
    red_one.pair_send()
    grads = (red_two, red_one)
    for red in grads:
        for s in range(2):
            red.pair_sum(s)
            red.first_send(s)
    dpre.frame_wait()
    transposed(one, one_t)
    dpre.windows(1)
    dpre.middle(one_t, out_v)
    for red in grads:
        for s in range(2):
            red.first_sum(s)
            red.second_send(s)
    dpre.bulk_send(0)
    dpre.bulk_send(1)
    dpre.rim_send()
    for red in grads:
        for s in range(2):
            red.second_sum(s)
            red.third_send(s)
    for red in grads:
        for s in range(2):
            red.third_sum(s)
            red.third_gather(s)
    dpre.times_wait()
    dpre.windows(0)
    dpre.windows(2)
    dpre.outer(one_t, out_v)

    def finish(g, _):
        row = 4 * g
        d_vol[pl.ds(row, 4)] = shifted(out_v, row).astype(BF16)
        return 0

    lax.fori_loop(0, 8, finish, 0)
    for red in grads:
        for s in range(2):
            red.second_gather(s)
    for red in grads:
        for s in range(2):
            red.first_gather(s)
    for red in grads:
        for s in range(2):
            red.pair_gather(s)
    for red in grads:
        for s in range(2):
            red.finish(s)
            red.drain(s)
    for field in (vol, cot, dpre):
        field.drain()


def scale_kernel(scale, full_one, full_two, d_in, grad_one, grad_two, d_out, buf, sems):
    through = pltpu.make_async_copy(d_in, d_out, sems.at[2])
    through.start()
    for g, (full, grad) in enumerate(((full_two, grad_two), (full_one, grad_one))):

        def step(tap, _):
            tiles = full[:, tap + 2 * (tap // 14)].astype(F32) * scale
            buf[g, tap] = tiles.reshape(128, 128)
            pltpu.make_async_copy(buf.at[g, tap], grad.at[tap], sems.at[g]).start()
            return 0

        lax.fori_loop(0, 27, step, 0)
    through.wait()
    wait_bytes(buf.at[0], sems.at[0])
    wait_bytes(buf.at[1], sems.at[1])


def in_hbm(array):
    return pltpu.with_memory_space_constraint(array, pltpu.HBM)


def body(volume, cotangent, kernel_one, kernel_two):
    total_cells = (
        volume.shape[0]
        * volume.shape[1]
        * volume.shape[2]
        * lax.axis_size("ta")
        * lax.axis_size("ha")
        * lax.axis_size("wa")
    )
    scale = float(1.0 / np.sqrt(np.float32(total_cells)))
    full = jax.ShapeDtypeStruct((8, 32, 16, 128), BF16)
    taps = pltpu.VMEM((27, 128, 128), BF16)
    d_volume, full_one, full_two = pl.pallas_call(
        block_kernel,
        out_shape=(jax.ShapeDtypeStruct((32, 16, 128), BF16), full, full),
        in_specs=[pl.BlockSpec(memory_space=pltpu.HBM)] * 4,
        out_specs=[pl.BlockSpec(memory_space=pltpu.VMEM)] * 3,
        scratch_shapes=FIELD_SCRATCH * 3
        + [pltpu.VMEM((8, 32, 16, 128), BF16)] * 2
        + REDUCE_SCRATCH * 2
        + [taps] * 4
        + [pltpu.VMEM((34, 16, 384), F32)] * 2
        + [
            pltpu.VMEM((32, 16, 128), F32),
            pltpu.VMEM((32, 16, 128), BF16),
            pltpu.VMEM((128, 512), BF16),
            pltpu.SemaphoreType.DMA((4,)),
        ],
        compiler_params=pltpu.CompilerParams(
            collective_id=0, has_side_effects=True, vmem_limit_bytes=32 * 1024 * 1024
        ),
    )(
        in_hbm(volume.reshape(32, 16, 128)),
        in_hbm(cotangent.reshape(32, 16, 128)),
        in_hbm(kernel_one.reshape(27, 128, 128)),
        in_hbm(kernel_two.reshape(27, 128, 128)),
    )
    grad = jax.ShapeDtypeStruct((27, 128, 128), F32)
    grad_one, grad_two, d_volume = pl.pallas_call(
        functools.partial(scale_kernel, scale),
        out_shape=(grad, grad, jax.ShapeDtypeStruct((32, 16, 128), BF16)),
        in_specs=[pl.BlockSpec(memory_space=pltpu.VMEM)] * 3,
        out_specs=[pl.BlockSpec(memory_space=pl.ANY)] * 3,
        scratch_shapes=[pltpu.VMEM((2, 27, 128, 128), F32), pltpu.SemaphoreType.DMA((3,))],
        compiler_params=pltpu.CompilerParams(vmem_limit_bytes=16 * 1024 * 1024),
    )(full_one, full_two, d_volume)
    return (
        d_volume.reshape(volume.shape),
        grad_one.reshape(kernel_one.shape),
        grad_two.reshape(kernel_two.shape),
    )


def solution(mesh):
    in_specs = (P("ta", "ha", "wa", None), P("ta", "ha", "wa", None), P(), P())
    out_specs = (P("ta", "ha", "wa", None), P(), P())
    return jax.shard_map(body, mesh=mesh, in_specs=in_specs, out_specs=out_specs, check_vma=False)
```

```python
import functools

import jax
import jax.numpy as jnp
import numpy as np
from jax import lax
from jax.experimental import pallas as pl
from jax.experimental.pallas import tpu as pltpu
from jax.sharding import PartitionSpec as P

MESH = pl.DeviceIdType.MESH
F32 = jnp.float32
BF16 = jnp.bfloat16


class Place:
    def __init__(self):
        self.ta = lax.axis_index("ta")
        self.ha = lax.axis_index("ha")
        self.wa = lax.axis_index("wa")
        self.core = lax.rem(self.wa, 2)
        self.x = lax.rem(self.ta, 4)
        self.y = self.ha
        self.z = (self.wa // 2) * 2 + self.ta // 4

    def peer_x(self, off):
        to = lax.rem(self.x + off, 4)
        return to, (self.ta - self.x + to, self.ha, self.wa)

    def peer_y(self, off):
        to = lax.rem(self.y + off, 4)
        return to, (self.ta, to, self.wa)

    def peer_z(self, off):
        to = lax.rem(self.z + off, 8)
        return to, (lax.rem(to, 2) * 4 + self.x, self.ha, (to // 2) * 2 + self.core)

    def near(self, dta, dha, dwa):
        return (lax.rem(self.ta + dta + 8, 8), lax.rem(self.ha + dha + 4, 4), lax.rem(self.wa + dwa + 8, 8))

    def twin(self):
        return (self.ta, self.ha, self.wa + 1 - 2 * self.core)


def send(src, dst, send_sem, recv_sem, device):
    pltpu.make_async_remote_copy(
        src_ref=src, dst_ref=dst, send_sem=send_sem, recv_sem=recv_sem,
        device_id=device, device_id_type=MESH,
    ).start()


def wait_bytes(ref, sem):
    pltpu.make_async_copy(ref, ref, sem).wait()


PHASES = 7


class Reduce:
    def __init__(self, place, part, full, land0, sums, land1, tops, land2, thirds, sends, recvs):
        self.at = place
        self.part, self.full = part, full
        self.land0, self.sums, self.land1 = land0, sums, land1
        self.tops, self.land2, self.thirds = tops, land2, thirds
        self.sends, self.recvs = sends, recvs

    def first(self, s, off):
        return self.at.peer_x(off) if s == 0 else self.at.peer_y(off)

    def last(self, s, off):
        return self.at.peer_y(off) if s == 0 else self.at.peer_x(off)

    def mine(self, s):
        return (self.at.x, self.at.y) if s == 0 else (self.at.y, self.at.x)

    def go(self, phase, s, src, dst, device):
        send(src, dst, self.sends.at[phase, s], self.recvs.at[phase, s], device)

    def pair_send(self):
        other = 4 - 4 * self.at.core
        for s in range(2):
            self.go(0, s, self.part.at[pl.ds(other, 4), pl.ds(16 * s, 14)], self.land0.at[s], self.at.twin())

    def pair_sum(self, s):
        own = 4 * self.at.core
        wait_bytes(self.land0.at[s], self.recvs.at[0, s])

        def step(i, _):
            total = self.part[own + i, pl.ds(16 * s, 14)].astype(F32) + self.land0[s, i].astype(F32)
            self.sums[s, i] = total.astype(BF16)
            return 0

        lax.fori_loop(0, 4, step, 0)

    def first_send(self, s):
        for off in range(1, 4):
            to, device = self.first(s, off)
            self.go(1, s, self.sums.at[s, to], self.land1.at[s, off - 1], device)

    def first_sum(self, s):
        me, _ = self.mine(s)
        wait_bytes(self.land1.at[s], self.recvs.at[1, s])
        total = self.sums[s, me].astype(F32)
        for j in range(3):
            total = total + self.land1[s, j].astype(F32)
        self.tops[s, pl.ds(0, 14)] = total.astype(BF16)
        self.tops[s, pl.ds(14, 2)] = jnp.zeros((2, 16, 128), BF16)

    def second_send(self, s):
        for off in range(1, 8):
            to, device = self.at.peer_z(off)
            self.go(2, s, self.tops.at[s, pl.ds(2 * to, 2)], self.land2.at[s, off - 1], device)

    def second_sum(self, s):
        _, me = self.mine(s)
        wait_bytes(self.land2.at[s], self.recvs.at[2, s])
        total = self.tops[s, pl.ds(2 * self.at.z, 2)].astype(F32)
        for j in range(7):
            total = total + self.land2[s, j].astype(F32)
        self.thirds[s, me] = total.astype(BF16)

    def third_send(self, s):
        _, me = self.mine(s)
        for off in range(1, 4):
            _, device = self.last(s, off)
            self.go(3, s, self.thirds.at[s, me], self.thirds.at[s, me], device)

    def spot(self, s):
        me, _ = self.mine(s)
        return 4 * self.at.core + me, pl.ds(16 * s + 2 * self.at.z, 2)

    def third_sum(self, s):
        wait_bytes(self.thirds.at[s, pl.ds(0, 3)], self.recvs.at[3, s])
        total = self.thirds[s, 0].astype(F32)
        for j in range(1, 4):
            total = total + self.thirds[s, j].astype(F32)
        row, slots = self.spot(s)
        self.full[row, slots] = total.astype(BF16)

    def second_gather(self, s):
        row, slots = self.spot(s)
        for off in range(1, 8):
            _, device = self.at.peer_z(off)
            self.go(4, s, self.full.at[row, slots], self.full.at[row, slots], device)

    def first_gather(self, s):
        me, _ = self.mine(s)
        wait_bytes(self.full.at[0, pl.ds(0, 14)], self.recvs.at[4, s])
        row = 4 * self.at.core + me
        slots = pl.ds(16 * s, 14)
        for off in range(1, 4):
            _, device = self.first(s, off)
            self.go(5, s, self.full.at[row, slots], self.full.at[row, slots], device)

    def pair_gather(self, s):
        wait_bytes(self.full.at[pl.ds(0, 3), pl.ds(0, 14)], self.recvs.at[5, s])
        rows = pl.ds(4 * self.at.core, 4)
        slots = pl.ds(16 * s, 14)
        self.go(6, s, self.full.at[rows, slots], self.full.at[rows, slots], self.at.twin())

    def finish(self, s):
        wait_bytes(self.full.at[pl.ds(0, 4), pl.ds(0, 14)], self.recvs.at[6, s])

    def drain(self, s):
        wait_bytes(self.land0.at[s], self.sends.at[0, s])
        wait_bytes(self.land1.at[s], self.sends.at[1, s])
        wait_bytes(self.land2.at[s], self.sends.at[2, s])
        wait_bytes(self.thirds.at[s, pl.ds(0, 3)], self.sends.at[3, s])
        wait_bytes(self.full.at[0, pl.ds(0, 14)], self.sends.at[4, s])
        wait_bytes(self.full.at[pl.ds(0, 3), pl.ds(0, 14)], self.sends.at[5, s])
        wait_bytes(self.full.at[pl.ds(0, 4), pl.ds(0, 14)], self.sends.at[6, s])


REDUCE_SCRATCH = [
    pltpu.VMEM((2, 4, 14, 16, 128), BF16),
    pltpu.VMEM((2, 4, 14, 16, 128), BF16),
    pltpu.VMEM((2, 3, 14, 16, 128), BF16),
    pltpu.VMEM((2, 16, 16, 128), BF16),
    pltpu.VMEM((2, 7, 2, 16, 128), BF16),
    pltpu.VMEM((2, 4, 2, 16, 128), BF16),
    pltpu.SemaphoreType.DMA((PHASES, 2)),
    pltpu.SemaphoreType.DMA((PHASES, 2)),
]


def reduce_peers(place):
    peers = [place.twin()]
    peers += [place.peer_x(off)[1] for off in range(1, 4)]
    peers += [place.peer_y(off)[1] for off in range(1, 4)]
    peers += [place.peer_z(off)[1] for off in range(1, 8)]
    return peers


class Field:
    def __init__(self, place, raw, wide, cols, ends, cols_out, ends_out, win, sends, recvs):
        self.at = place
        self.raw, self.wide = raw, wide
        self.cols, self.ends, self.cols_out, self.ends_out = cols, ends, cols_out, ends_out
        self.win, self.sends, self.recvs = win, sends, recvs

    def stage(self):
        own = self.raw[1, pl.ds(1, 32)].astype(F32)
        self.wide[...] = own.reshape(512, 128)
        self.cols_out[0] = self.wide[pl.ds(0, 32, stride=16), :].astype(BF16)
        self.cols_out[1] = self.wide[pl.ds(15, 32, stride=16), :].astype(BF16)
        self.ends_out[0] = self.wide[pl.ds(0, 1), :]
        self.ends_out[1] = self.wide[pl.ds(496, 1), :]
        self.ends_out[2] = self.wide[pl.ds(15, 1), :]
        self.ends_out[3] = self.wide[pl.ds(511, 1), :]

    def go(self, kind, src, dst, device):
        send(src, dst, self.sends.at[kind], self.recvs.at[kind], device)

    def frame_send(self):
        near = self.at.near
        self.go(0, self.raw.at[1, 1], self.raw.at[1, 33], near(0, -1, 0))
        self.go(0, self.raw.at[1, 32], self.raw.at[1, 0], near(0, 1, 0))
        self.go(1, self.cols_out.at[0], self.cols.at[1, 1], near(0, 0, -1))
        self.go(1, self.cols_out.at[1], self.cols.at[1, 0], near(0, 0, 1))
        self.go(2, self.ends_out.at[0], self.ends.at[1, 3], near(0, -1, -1))
        self.go(2, self.ends_out.at[1], self.ends.at[1, 2], near(0, 1, -1))
        self.go(2, self.ends_out.at[2], self.ends.at[1, 1], near(0, -1, 1))
        self.go(2, self.ends_out.at[3], self.ends.at[1, 0], near(0, 1, 1))

    def bulk_send(self, half):
        near = self.at.near
        rows = pl.ds(1 + 16 * half, 16)
        own = self.raw.at[1, rows]
        self.go(3, own, self.raw.at[0, rows], near(1, 0, 0))
        self.go(3, own, self.raw.at[2, rows], near(-1, 0, 0))

    def frame_wait(self):
        wait_bytes(self.raw.at[1, pl.ds(0, 2)], self.recvs.at[0])
        wait_bytes(self.cols.at[1], self.recvs.at[1])
        wait_bytes(self.ends.at[1], self.recvs.at[2])

    def rim_send(self):
        for frame, step in ((0, 1), (2, -1)):
            device = self.at.near(step, 0, 0)
            self.go(4, self.raw.at[1, 0], self.raw.at[frame, 0], device)
            self.go(4, self.raw.at[1, 33], self.raw.at[frame, 33], device)
            self.go(5, self.cols.at[1], self.cols.at[frame], device)
            self.go(6, self.ends.at[1], self.ends.at[frame], device)

    def times_wait(self):
        wait_bytes(self.raw.at[pl.ds(0, 2), pl.ds(0, 32)], self.recvs.at[3])
        wait_bytes(self.raw.at[0, pl.ds(0, 4)], self.recvs.at[4])
        wait_bytes(self.cols.at[pl.ds(0, 2)], self.recvs.at[5])
        wait_bytes(self.ends.at[pl.ds(0, 2)], self.recvs.at[6])

    def drain(self):
        wait_bytes(self.raw.at[1, pl.ds(0, 2)], self.sends.at[0])
        wait_bytes(self.cols.at[1], self.sends.at[1])
        wait_bytes(self.ends.at[1], self.sends.at[2])
        wait_bytes(self.raw.at[pl.ds(0, 2), pl.ds(0, 32)], self.sends.at[3])
        wait_bytes(self.raw.at[0, pl.ds(0, 4)], self.sends.at[4])
        wait_bytes(self.cols.at[pl.ds(0, 2)], self.sends.at[5])
        wait_bytes(self.ends.at[pl.ds(0, 2)], self.sends.at[6])

    def windows(self, frame):
        spot = lax.broadcasted_iota(jnp.int32, (16, 128), 0)
        at_left, at_right = self.at.wa == 0, self.at.wa == 7

        def line(row, left, right):
            mid = self.raw[frame, row]
            wide = mid.astype(F32)
            left = jnp.where(at_left, 0.0, left)
            right = jnp.where(at_right, 0.0, right)
            before = jnp.where(spot == 0, left, pltpu.roll(wide, 1, 0))
            after = jnp.where(spot == 15, right, pltpu.roll(wide, 15, 0))
            self.win[frame, row, :, pl.ds(0, 128)] = before.astype(BF16)
            self.win[frame, row, :, pl.ds(128, 128)] = mid
            self.win[frame, row, :, pl.ds(256, 128)] = after.astype(BF16)

        def group(g, _):
            start = pl.multiple_of(16 * g, 16)
            left = self.cols[frame, 0, pl.ds(start, 16), :].astype(F32)
            right = self.cols[frame, 1, pl.ds(start, 16), :].astype(F32)
            for r in range(16):
                line(16 * g + r + 1, left[r : r + 1], right[r : r + 1])
            return 0

        lax.fori_loop(0, 2, group, 0)
        line(0, self.ends[frame, 0], self.ends[frame, 2])
        line(33, self.ends[frame, 1], self.ends[frame, 3])
        blank = jnp.zeros((16, 384), BF16)

        @pl.when(self.at.ha == 0)
        def _():
            self.win[frame, 0] = blank

        @pl.when(self.at.ha == 3)
        def _():
            self.win[frame, 33] = blank

        if frame != 1:

            @pl.when(self.at.ta == (0 if frame == 0 else 7))
            def _():
                self.win[frame] = jnp.zeros((34, 16, 384), BF16)

    def taps(self, weights, frame):
        rows = [weights[pl.ds(9 * frame + 3 * kh, 3)].reshape(384, 128) for kh in range(3)]
        return jnp.concatenate(rows, axis=1)

    def middle(self, weights, out):
        lhs = self.win[1].reshape(544, 384)
        out[...] = jnp.dot(lhs, self.taps(weights, 1), preferred_element_type=F32).reshape(34, 16, 384)

    def outer(self, weights, out):
        lhs = jnp.concatenate([self.win[0].reshape(544, 384), self.win[2].reshape(544, 384)], axis=1)
        rhs = jnp.concatenate([self.taps(weights, 0), self.taps(weights, 2)], axis=0)
        out[...] = out[...] + jnp.dot(lhs, rhs, preferred_element_type=F32).reshape(34, 16, 384)


FIELD_SCRATCH = [
    pltpu.VMEM((3, 34, 16, 128), BF16),
    pltpu.VMEM((512, 128), F32),
    pltpu.VMEM((3, 2, 32, 128), BF16),
    pltpu.VMEM((3, 4, 1, 128), F32),
    pltpu.VMEM((2, 32, 128), BF16),
    pltpu.VMEM((4, 1, 128), F32),
    pltpu.VMEM((3, 34, 16, 384), BF16),
    pltpu.SemaphoreType.DMA((7,)),
    pltpu.SemaphoreType.DMA((7,)),
]


def shifted(out, row):
    return (
        out[pl.ds(row, 4), :, pl.ds(0, 128)]
        + out[pl.ds(row + 1, 4), :, pl.ds(128, 128)]
        + out[pl.ds(row + 2, 4), :, pl.ds(256, 128)]
    )


def slot_of(tap):
    return tap if tap < 14 else tap + 2


def transposed(weights, out):
    def step(n, _):
        out[n] = weights[26 - n].T
        return 0

    lax.fori_loop(0, 27, step, 0)


def block_kernel(vol_hbm, cot_hbm, one_hbm, two_hbm, d_vol, full_one, full_two, *scratch):
    place = Place()
    barrier = pltpu.get_barrier_semaphore()
    others = reduce_peers(place)
    others += [place.near(s, 0, 0) for s in (1, -1)]
    others += [place.near(0, 0, s) for s in (1, -1)]
    others += [place.near(0, a, b) for a in (1, -1) for b in (1, -1)]
    for device in others:
        pl.semaphore_signal(barrier, inc=1, device_id=device, device_id_type=MESH)

    f, r = len(FIELD_SCRATCH), len(REDUCE_SCRATCH)
    vol = Field(place, *scratch[:f])
    cot = Field(place, *scratch[f : 2 * f])
    dpre = Field(place, *scratch[2 * f : 3 * f])
    scratch = scratch[3 * f :]
    part_one, part_two = scratch[0], scratch[1]
    red_two = Reduce(place, part_two, full_two, *scratch[2 : 2 + r])
    red_one = Reduce(place, part_one, full_one, *scratch[2 + r : 2 + 2 * r])
    scratch = scratch[2 + 2 * r :]
    one, two, one_t, two_t, out_v, out_c, gate, act, act_t, local = scratch

    loads = [
        pltpu.make_async_copy(vol_hbm, vol.raw.at[1, pl.ds(1, 32)], local.at[0]),
        pltpu.make_async_copy(cot_hbm, cot.raw.at[1, pl.ds(1, 32)], local.at[1]),
        pltpu.make_async_copy(two_hbm, two, local.at[2]),
        pltpu.make_async_copy(one_hbm, one, local.at[3]),
    ]
    for load in loads:
        load.start()
    part_one[:, 29] = jnp.zeros((8, 16, 128), BF16)
    part_two[:, 29] = jnp.zeros((8, 16, 128), BF16)
    loads[0].wait()
    vol.stage()
    loads[1].wait()
    cot.stage()
    pl.semaphore_wait(barrier, len(others))

    vol.frame_send()
    vol.bulk_send(0)
    vol.bulk_send(1)
    cot.frame_send()
    cot.bulk_send(0)
    loads[2].wait()
    transposed(two, two_t)
    loads[3].wait()
    vol.frame_wait()
    vol.rim_send()
    cot.bulk_send(1)
    cot.frame_wait()
    cot.rim_send()
    vol.windows(1)
    cot.windows(1)
    vol.middle(one, out_v)
    cot.middle(two_t, out_c)

    vol.times_wait()
    vol.windows(0)
    vol.windows(2)
    vol.outer(one, out_v)

    def activate(g, _):
        row = 4 * g
        pre = shifted(out_v, row)
        sig = 1.0 / (1.0 + jnp.exp(-pre))
        act[pl.ds(row, 4)] = (pre * sig).astype(BF16)
        gate[pl.ds(row, 4)] = sig * (1.0 + pre * (1.0 - sig))
        return 0

    lax.fori_loop(0, 8, activate, 0)
    act_t[...] = act[...].reshape(512, 128).T

    cot.times_wait()
    cot.windows(0)
    cot.windows(2)
    for t in range(3):
        for kh in range(3):
            rhs = cot.win[t, pl.ds(kh, 32)].reshape(512, 384)
            got = jnp.dot(act_t[...], rhs, preferred_element_type=F32)
            for kw in range(3):
                tap = 26 - (9 * t + 3 * kh + kw)
                block = got[:, 128 * kw : 128 * kw + 128].reshape(8, 16, 128)
                part_two[:, slot_of(tap)] = block.astype(BF16)
    red_two.pair_send()

    cot.outer(two_t, out_c)

    def backward(g, _):
        row = 4 * g
        dpre.raw[1, pl.ds(row + 1, 4)] = (shifted(out_c, row) * gate[pl.ds(row, 4)]).astype(BF16)
        return 0

    lax.fori_loop(0, 8, backward, 0)
    dpre.stage()
    dpre.frame_send()
    act_t[...] = dpre.raw[1, pl.ds(1, 32)].reshape(512, 128).T
    for t in range(3):
        for kh in range(3):
            rhs = vol.win[t, pl.ds(kh, 32)].reshape(512, 384)
            got = jnp.dot(act_t[...], rhs, preferred_element_type=F32)
            for kw in range(3):
                tap = 9 * t + 3 * kh + kw
                block = got[:, 128 * kw : 128 * kw + 128].T.reshape(8, 16, 128)
                part_one[:, slot_of(tap)] = block.astype(BF16)
    red_one.pair_send()
    grads = (red_two, red_one)
    for red in grads:
        for s in range(2):
            red.pair_sum(s)
            red.first_send(s)
    dpre.frame_wait()
    transposed(one, one_t)
    dpre.windows(1)
    dpre.middle(one_t, out_v)
    for red in grads:
        for s in range(2):
            red.first_sum(s)
            red.second_send(s)
    dpre.bulk_send(0)
    dpre.bulk_send(1)
    dpre.rim_send()
    for red in grads:
        for s in range(2):
            red.second_sum(s)
            red.third_send(s)
    for red in grads:
        for s in range(2):
            red.third_sum(s)
            red.second_gather(s)
    dpre.times_wait()
    dpre.windows(0)
    dpre.windows(2)
    dpre.outer(one_t, out_v)

    def finish(g, _):
        row = 4 * g
        d_vol[pl.ds(row, 4)] = shifted(out_v, row).astype(BF16)
        return 0

    lax.fori_loop(0, 8, finish, 0)
    for red in grads:
        for s in range(2):
            red.first_gather(s)
    for red in grads:
        for s in range(2):
            red.pair_gather(s)
    for red in grads:
        for s in range(2):
            red.finish(s)
            red.drain(s)
    for field in (vol, cot, dpre):
        field.drain()


def scale_kernel(scale, full_one, full_two, d_in, grad_one, grad_two, d_out, buf, sems):
    through = pltpu.make_async_copy(d_in, d_out, sems.at[2])
    through.start()
    for g, (full, grad) in enumerate(((full_two, grad_two), (full_one, grad_one))):

        def step(tap, _):
            tiles = full[:, tap + 2 * (tap // 14)].astype(F32) * scale
            buf[g, tap] = tiles.reshape(128, 128)
            pltpu.make_async_copy(buf.at[g, tap], grad.at[tap], sems.at[g]).start()
            return 0

        lax.fori_loop(0, 27, step, 0)
    through.wait()
    wait_bytes(buf.at[0], sems.at[0])
    wait_bytes(buf.at[1], sems.at[1])


def in_hbm(array):
    return pltpu.with_memory_space_constraint(array, pltpu.HBM)


def body(volume, cotangent, kernel_one, kernel_two):
    total_cells = (
        volume.shape[0]
        * volume.shape[1]
        * volume.shape[2]
        * lax.axis_size("ta")
        * lax.axis_size("ha")
        * lax.axis_size("wa")
    )
    scale = float(1.0 / np.sqrt(np.float32(total_cells)))
    full = jax.ShapeDtypeStruct((8, 32, 16, 128), BF16)
    taps = pltpu.VMEM((27, 128, 128), BF16)
    d_volume, full_one, full_two = pl.pallas_call(
        block_kernel,
        out_shape=(jax.ShapeDtypeStruct((32, 16, 128), BF16), full, full),
        in_specs=[pl.BlockSpec(memory_space=pltpu.HBM)] * 4,
        out_specs=[pl.BlockSpec(memory_space=pltpu.VMEM)] * 3,
        scratch_shapes=FIELD_SCRATCH * 3
        + [pltpu.VMEM((8, 32, 16, 128), BF16)] * 2
        + REDUCE_SCRATCH * 2
        + [taps] * 4
        + [pltpu.VMEM((34, 16, 384), F32)] * 2
        + [
            pltpu.VMEM((32, 16, 128), F32),
            pltpu.VMEM((32, 16, 128), BF16),
            pltpu.VMEM((128, 512), BF16),
            pltpu.SemaphoreType.DMA((4,)),
        ],
        compiler_params=pltpu.CompilerParams(
            collective_id=0, has_side_effects=True, vmem_limit_bytes=32 * 1024 * 1024
        ),
    )(
        in_hbm(volume.reshape(32, 16, 128)),
        in_hbm(cotangent.reshape(32, 16, 128)),
        in_hbm(kernel_one.reshape(27, 128, 128)),
        in_hbm(kernel_two.reshape(27, 128, 128)),
    )
    grad = jax.ShapeDtypeStruct((27, 128, 128), F32)
    grad_one, grad_two, d_volume = pl.pallas_call(
        functools.partial(scale_kernel, scale),
        out_shape=(grad, grad, jax.ShapeDtypeStruct((32, 16, 128), BF16)),
        in_specs=[pl.BlockSpec(memory_space=pltpu.VMEM)] * 3,
        out_specs=[pl.BlockSpec(memory_space=pl.ANY)] * 3,
        scratch_shapes=[pltpu.VMEM((2, 27, 128, 128), F32), pltpu.SemaphoreType.DMA((3,))],
        compiler_params=pltpu.CompilerParams(vmem_limit_bytes=16 * 1024 * 1024),
    )(full_one, full_two, d_volume)
    return (
        d_volume.reshape(volume.shape),
        grad_one.reshape(kernel_one.shape),
        grad_two.reshape(kernel_two.shape),
    )


def solution(mesh):
    in_specs = (P("ta", "ha", "wa", None), P("ta", "ha", "wa", None), P(), P())
    out_specs = (P("ta", "ha", "wa", None), P(), P())
    return jax.shard_map(body, mesh=mesh, in_specs=in_specs, out_specs=out_specs, check_vma=False)
```

```python
import functools

import jax
import jax.numpy as jnp
import numpy as np
from jax import lax
from jax.experimental import pallas as pl
from jax.experimental.pallas import tpu as pltpu
from jax.sharding import PartitionSpec as P

MESH = pl.DeviceIdType.MESH
F32 = jnp.float32
BF16 = jnp.bfloat16


class Place:
    def __init__(self):
        self.ta = lax.axis_index("ta")
        self.ha = lax.axis_index("ha")
        self.wa = lax.axis_index("wa")
        self.core = lax.rem(self.wa, 2)
        self.x = lax.rem(self.ta, 4)
        self.y = self.ha
        self.z = (self.wa // 2) * 2 + self.ta // 4

    def peer_x(self, off):
        to = lax.rem(self.x + off, 4)
        return to, (self.ta - self.x + to, self.ha, self.wa)

    def peer_y(self, off):
        to = lax.rem(self.y + off, 4)
        return to, (self.ta, to, self.wa)

    def peer_z(self, off):
        to = lax.rem(self.z + off, 8)
        return to, (lax.rem(to, 2) * 4 + self.x, self.ha, (to // 2) * 2 + self.core)

    def near(self, dta, dha, dwa):
        return (lax.rem(self.ta + dta + 8, 8), lax.rem(self.ha + dha + 4, 4), lax.rem(self.wa + dwa + 8, 8))

    def twin(self):
        return (self.ta, self.ha, self.wa + 1 - 2 * self.core)


def send(src, dst, send_sem, recv_sem, device):
    pltpu.make_async_remote_copy(
        src_ref=src, dst_ref=dst, send_sem=send_sem, recv_sem=recv_sem,
        device_id=device, device_id_type=MESH,
    ).start()


def wait_bytes(ref, sem):
    pltpu.make_async_copy(ref, ref, sem).wait()


PHASES = 7


class Reduce:
    def __init__(self, place, part, full, land0, sums, land1, tops, land2, thirds, sends, recvs):
        self.at = place
        self.part, self.full = part, full
        self.land0, self.sums, self.land1 = land0, sums, land1
        self.tops, self.land2, self.thirds = tops, land2, thirds
        self.sends, self.recvs = sends, recvs

    def first(self, s, off):
        return self.at.peer_x(off) if s == 0 else self.at.peer_y(off)

    def last(self, s, off):
        return self.at.peer_y(off) if s == 0 else self.at.peer_x(off)

    def mine(self, s):
        return (self.at.x, self.at.y) if s == 0 else (self.at.y, self.at.x)

    def go(self, phase, s, src, dst, device):
        send(src, dst, self.sends.at[phase, s], self.recvs.at[phase, s], device)

    def pair_send(self):
        other = 4 - 4 * self.at.core
        for s in range(2):
            self.go(0, s, self.part.at[pl.ds(other, 4), pl.ds(16 * s, 14)], self.land0.at[s], self.at.twin())

    def pair_sum(self, s):
        own = 4 * self.at.core
        wait_bytes(self.land0.at[s], self.recvs.at[0, s])

        def step(i, _):
            total = self.part[own + i, pl.ds(16 * s, 14)].astype(F32) + self.land0[s, i].astype(F32)
            self.sums[s, i] = total.astype(BF16)
            return 0

        lax.fori_loop(0, 4, step, 0)

    def first_send(self, s):
        for off in range(1, 4):
            to, device = self.first(s, off)
            self.go(1, s, self.sums.at[s, to], self.land1.at[s, off - 1], device)

    def first_sum(self, s):
        me, _ = self.mine(s)
        wait_bytes(self.land1.at[s], self.recvs.at[1, s])
        total = self.sums[s, me].astype(F32)
        for j in range(3):
            total = total + self.land1[s, j].astype(F32)
        self.tops[s, pl.ds(0, 14)] = total.astype(BF16)
        self.tops[s, pl.ds(14, 2)] = jnp.zeros((2, 16, 128), BF16)

    def second_send(self, s):
        for off in (4, 3, 5, 2, 6, 1, 7):
            to, device = self.at.peer_z(off)
            self.go(2, s, self.tops.at[s, pl.ds(2 * to, 2)], self.land2.at[s, off - 1], device)

    def second_sum(self, s):
        _, me = self.mine(s)
        wait_bytes(self.land2.at[s], self.recvs.at[2, s])
        total = self.tops[s, pl.ds(2 * self.at.z, 2)].astype(F32)
        for j in range(7):
            total = total + self.land2[s, j].astype(F32)
        self.thirds[s, me] = total.astype(BF16)

    def third_send(self, s):
        _, me = self.mine(s)
        for off in range(1, 4):
            _, device = self.last(s, off)
            self.go(3, s, self.thirds.at[s, me], self.thirds.at[s, me], device)

    def spot(self, s):
        me, _ = self.mine(s)
        return 4 * self.at.core + me, pl.ds(16 * s + 2 * self.at.z, 2)

    def third_sum(self, s):
        wait_bytes(self.thirds.at[s, pl.ds(0, 3)], self.recvs.at[3, s])
        total = self.thirds[s, 0].astype(F32)
        for j in range(1, 4):
            total = total + self.thirds[s, j].astype(F32)
        row, slots = self.spot(s)
        self.full[row, slots] = total.astype(BF16)

    def second_gather(self, s):
        row, slots = self.spot(s)
        for off in (4, 3, 5, 2, 6, 1, 7):
            _, device = self.at.peer_z(off)
            self.go(4, s, self.full.at[row, slots], self.full.at[row, slots], device)

    def first_gather(self, s):
        me, _ = self.mine(s)
        wait_bytes(self.full.at[0, pl.ds(0, 14)], self.recvs.at[4, s])
        row = 4 * self.at.core + me
        slots = pl.ds(16 * s, 14)
        for off in range(1, 4):
            _, device = self.first(s, off)
            self.go(5, s, self.full.at[row, slots], self.full.at[row, slots], device)

    def pair_gather(self, s):
        wait_bytes(self.full.at[pl.ds(0, 3), pl.ds(0, 14)], self.recvs.at[5, s])
        rows = pl.ds(4 * self.at.core, 4)
        slots = pl.ds(16 * s, 14)
        self.go(6, s, self.full.at[rows, slots], self.full.at[rows, slots], self.at.twin())

    def finish(self, s):
        wait_bytes(self.full.at[pl.ds(0, 4), pl.ds(0, 14)], self.recvs.at[6, s])

    def drain(self, s):
        wait_bytes(self.land0.at[s], self.sends.at[0, s])
        wait_bytes(self.land1.at[s], self.sends.at[1, s])
        wait_bytes(self.land2.at[s], self.sends.at[2, s])
        wait_bytes(self.thirds.at[s, pl.ds(0, 3)], self.sends.at[3, s])
        wait_bytes(self.full.at[0, pl.ds(0, 14)], self.sends.at[4, s])
        wait_bytes(self.full.at[pl.ds(0, 3), pl.ds(0, 14)], self.sends.at[5, s])
        wait_bytes(self.full.at[pl.ds(0, 4), pl.ds(0, 14)], self.sends.at[6, s])


REDUCE_SCRATCH = [
    pltpu.VMEM((2, 4, 14, 16, 128), BF16),
    pltpu.VMEM((2, 4, 14, 16, 128), BF16),
    pltpu.VMEM((2, 3, 14, 16, 128), BF16),
    pltpu.VMEM((2, 16, 16, 128), BF16),
    pltpu.VMEM((2, 7, 2, 16, 128), BF16),
    pltpu.VMEM((2, 4, 2, 16, 128), BF16),
    pltpu.SemaphoreType.DMA((PHASES, 2)),
    pltpu.SemaphoreType.DMA((PHASES, 2)),
]


def reduce_peers(place):
    peers = [place.twin()]
    peers += [place.peer_x(off)[1] for off in range(1, 4)]
    peers += [place.peer_y(off)[1] for off in range(1, 4)]
    peers += [place.peer_z(off)[1] for off in range(1, 8)]
    return peers


class Field:
    def __init__(self, place, raw, wide, cols, ends, cols_out, ends_out, win, sends, recvs):
        self.at = place
        self.raw, self.wide = raw, wide
        self.cols, self.ends, self.cols_out, self.ends_out = cols, ends, cols_out, ends_out
        self.win, self.sends, self.recvs = win, sends, recvs

    def stage(self):
        own = self.raw[1, pl.ds(1, 32)].astype(F32)
        self.wide[...] = own.reshape(512, 128)
        self.cols_out[0] = self.wide[pl.ds(0, 32, stride=16), :].astype(BF16)
        self.cols_out[1] = self.wide[pl.ds(15, 32, stride=16), :].astype(BF16)
        self.ends_out[0] = self.wide[pl.ds(0, 1), :]
        self.ends_out[1] = self.wide[pl.ds(496, 1), :]
        self.ends_out[2] = self.wide[pl.ds(15, 1), :]
        self.ends_out[3] = self.wide[pl.ds(511, 1), :]

    def go(self, kind, src, dst, device):
        send(src, dst, self.sends.at[kind], self.recvs.at[kind], device)

    def frame_send(self):
        near = self.at.near
        self.go(0, self.raw.at[1, 1], self.raw.at[1, 33], near(0, -1, 0))
        self.go(0, self.raw.at[1, 32], self.raw.at[1, 0], near(0, 1, 0))
        self.go(1, self.cols_out.at[0], self.cols.at[1, 1], near(0, 0, -1))
        self.go(1, self.cols_out.at[1], self.cols.at[1, 0], near(0, 0, 1))
        self.go(2, self.ends_out.at[0], self.ends.at[1, 3], near(0, -1, -1))
        self.go(2, self.ends_out.at[1], self.ends.at[1, 2], near(0, 1, -1))
        self.go(2, self.ends_out.at[2], self.ends.at[1, 1], near(0, -1, 1))
        self.go(2, self.ends_out.at[3], self.ends.at[1, 0], near(0, 1, 1))

    def bulk_send(self, half):
        near = self.at.near
        rows = pl.ds(1 + 16 * half, 16)
        own = self.raw.at[1, rows]
        self.go(3, own, self.raw.at[0, rows], near(1, 0, 0))
        self.go(3, own, self.raw.at[2, rows], near(-1, 0, 0))

    def frame_wait(self):
        wait_bytes(self.raw.at[1, pl.ds(0, 2)], self.recvs.at[0])
        wait_bytes(self.cols.at[1], self.recvs.at[1])
        wait_bytes(self.ends.at[1], self.recvs.at[2])

    def rim_send(self):
        for frame, step in ((0, 1), (2, -1)):
            device = self.at.near(step, 0, 0)
            self.go(4, self.raw.at[1, 0], self.raw.at[frame, 0], device)
            self.go(4, self.raw.at[1, 33], self.raw.at[frame, 33], device)
            self.go(5, self.cols.at[1], self.cols.at[frame], device)
            self.go(6, self.ends.at[1], self.ends.at[frame], device)

    def times_wait(self):
        wait_bytes(self.raw.at[pl.ds(0, 2), pl.ds(0, 32)], self.recvs.at[3])
        wait_bytes(self.raw.at[0, pl.ds(0, 4)], self.recvs.at[4])
        wait_bytes(self.cols.at[pl.ds(0, 2)], self.recvs.at[5])
        wait_bytes(self.ends.at[pl.ds(0, 2)], self.recvs.at[6])

    def drain(self):
        wait_bytes(self.raw.at[1, pl.ds(0, 2)], self.sends.at[0])
        wait_bytes(self.cols.at[1], self.sends.at[1])
        wait_bytes(self.ends.at[1], self.sends.at[2])
        wait_bytes(self.raw.at[pl.ds(0, 2), pl.ds(0, 32)], self.sends.at[3])
        wait_bytes(self.raw.at[0, pl.ds(0, 4)], self.sends.at[4])
        wait_bytes(self.cols.at[pl.ds(0, 2)], self.sends.at[5])
        wait_bytes(self.ends.at[pl.ds(0, 2)], self.sends.at[6])

    def windows(self, frame):
        spot = lax.broadcasted_iota(jnp.int32, (16, 128), 0)
        at_left, at_right = self.at.wa == 0, self.at.wa == 7

        def line(row, left, right):
            mid = self.raw[frame, row]
            wide = mid.astype(F32)
            left = jnp.where(at_left, 0.0, left)
            right = jnp.where(at_right, 0.0, right)
            before = jnp.where(spot == 0, left, pltpu.roll(wide, 1, 0))
            after = jnp.where(spot == 15, right, pltpu.roll(wide, 15, 0))
            self.win[frame, row, :, pl.ds(0, 128)] = before.astype(BF16)
            self.win[frame, row, :, pl.ds(128, 128)] = mid
            self.win[frame, row, :, pl.ds(256, 128)] = after.astype(BF16)

        def group(g, _):
            start = pl.multiple_of(16 * g, 16)
            left = self.cols[frame, 0, pl.ds(start, 16), :].astype(F32)
            right = self.cols[frame, 1, pl.ds(start, 16), :].astype(F32)
            for r in range(16):
                line(16 * g + r + 1, left[r : r + 1], right[r : r + 1])
            return 0

        lax.fori_loop(0, 2, group, 0)
        line(0, self.ends[frame, 0], self.ends[frame, 2])
        line(33, self.ends[frame, 1], self.ends[frame, 3])
        blank = jnp.zeros((16, 384), BF16)

        @pl.when(self.at.ha == 0)
        def _():
            self.win[frame, 0] = blank

        @pl.when(self.at.ha == 3)
        def _():
            self.win[frame, 33] = blank

        if frame != 1:

            @pl.when(self.at.ta == (0 if frame == 0 else 7))
            def _():
                self.win[frame] = jnp.zeros((34, 16, 384), BF16)

    def taps(self, weights, frame):
        rows = [weights[pl.ds(9 * frame + 3 * kh, 3)].reshape(384, 128) for kh in range(3)]
        return jnp.concatenate(rows, axis=1)

    def middle(self, weights, out):
        lhs = self.win[1].reshape(544, 384)
        out[...] = jnp.dot(lhs, self.taps(weights, 1), preferred_element_type=F32).reshape(34, 16, 384)

    def outer(self, weights, out):
        lhs = jnp.concatenate([self.win[0].reshape(544, 384), self.win[2].reshape(544, 384)], axis=1)
        rhs = jnp.concatenate([self.taps(weights, 0), self.taps(weights, 2)], axis=0)
        out[...] = out[...] + jnp.dot(lhs, rhs, preferred_element_type=F32).reshape(34, 16, 384)


FIELD_SCRATCH = [
    pltpu.VMEM((3, 34, 16, 128), BF16),
    pltpu.VMEM((512, 128), F32),
    pltpu.VMEM((3, 2, 32, 128), BF16),
    pltpu.VMEM((3, 4, 1, 128), F32),
    pltpu.VMEM((2, 32, 128), BF16),
    pltpu.VMEM((4, 1, 128), F32),
    pltpu.VMEM((3, 34, 16, 384), BF16),
    pltpu.SemaphoreType.DMA((7,)),
    pltpu.SemaphoreType.DMA((7,)),
]


def shifted(out, row):
    return (
        out[pl.ds(row, 4), :, pl.ds(0, 128)]
        + out[pl.ds(row + 1, 4), :, pl.ds(128, 128)]
        + out[pl.ds(row + 2, 4), :, pl.ds(256, 128)]
    )


def slot_of(tap):
    return tap if tap < 14 else tap + 2


def transposed(weights, out):
    def step(n, _):
        out[n] = weights[26 - n].T
        return 0

    lax.fori_loop(0, 27, step, 0)


def block_kernel(vol_hbm, cot_hbm, one_hbm, two_hbm, d_vol, full_one, full_two, *scratch):
    place = Place()
    barrier = pltpu.get_barrier_semaphore()
    others = reduce_peers(place)
    others += [place.near(s, 0, 0) for s in (1, -1)]
    others += [place.near(0, 0, s) for s in (1, -1)]
    others += [place.near(0, a, b) for a in (1, -1) for b in (1, -1)]
    for device in others:
        pl.semaphore_signal(barrier, inc=1, device_id=device, device_id_type=MESH)

    f, r = len(FIELD_SCRATCH), len(REDUCE_SCRATCH)
    vol = Field(place, *scratch[:f])
    cot = Field(place, *scratch[f : 2 * f])
    dpre = Field(place, *scratch[2 * f : 3 * f])
    scratch = scratch[3 * f :]
    part_one, part_two = scratch[0], scratch[1]
    red_two = Reduce(place, part_two, full_two, *scratch[2 : 2 + r])
    red_one = Reduce(place, part_one, full_one, *scratch[2 + r : 2 + 2 * r])
    scratch = scratch[2 + 2 * r :]
    one, two, one_t, two_t, out_v, out_c, gate, act, act_t, local = scratch

    loads = [
        pltpu.make_async_copy(vol_hbm, vol.raw.at[1, pl.ds(1, 32)], local.at[0]),
        pltpu.make_async_copy(cot_hbm, cot.raw.at[1, pl.ds(1, 32)], local.at[1]),
        pltpu.make_async_copy(two_hbm, two, local.at[2]),
        pltpu.make_async_copy(one_hbm, one, local.at[3]),
    ]
    for load in loads:
        load.start()
    part_one[:, 29] = jnp.zeros((8, 16, 128), BF16)
    part_two[:, 29] = jnp.zeros((8, 16, 128), BF16)
    loads[0].wait()
    vol.stage()
    loads[1].wait()
    cot.stage()
    pl.semaphore_wait(barrier, len(others))

    vol.frame_send()
    vol.bulk_send(0)
    vol.bulk_send(1)
    cot.frame_send()
    cot.bulk_send(0)
    loads[2].wait()
    transposed(two, two_t)
    loads[3].wait()
    vol.frame_wait()
    vol.rim_send()
    cot.bulk_send(1)
    cot.frame_wait()
    cot.rim_send()
    vol.windows(1)
    cot.windows(1)
    vol.middle(one, out_v)
    cot.middle(two_t, out_c)

    vol.times_wait()
    vol.windows(0)
    vol.windows(2)
    vol.outer(one, out_v)

    def activate(g, _):
        row = 4 * g
        pre = shifted(out_v, row)
        sig = 1.0 / (1.0 + jnp.exp(-pre))
        act[pl.ds(row, 4)] = (pre * sig).astype(BF16)
        gate[pl.ds(row, 4)] = sig * (1.0 + pre * (1.0 - sig))
        return 0

    lax.fori_loop(0, 8, activate, 0)
    act_t[...] = act[...].reshape(512, 128).T

    cot.times_wait()
    cot.windows(0)
    cot.windows(2)
    for t in range(3):
        for kh in range(3):
            rhs = cot.win[t, pl.ds(kh, 32)].reshape(512, 384)
            got = jnp.dot(act_t[...], rhs, preferred_element_type=F32)
            for kw in range(3):
                tap = 26 - (9 * t + 3 * kh + kw)
                block = got[:, 128 * kw : 128 * kw + 128].reshape(8, 16, 128)
                part_two[:, slot_of(tap)] = block.astype(BF16)
    red_two.pair_send()

    cot.outer(two_t, out_c)

    def backward(g, _):
        row = 4 * g
        dpre.raw[1, pl.ds(row + 1, 4)] = (shifted(out_c, row) * gate[pl.ds(row, 4)]).astype(BF16)
        return 0

    lax.fori_loop(0, 8, backward, 0)
    dpre.stage()
    dpre.frame_send()
    act_t[...] = dpre.raw[1, pl.ds(1, 32)].reshape(512, 128).T
    for s in range(2):
        red_two.pair_sum(s)
        red_two.first_send(s)
    for t in range(3):
        for kh in range(3):
            rhs = vol.win[t, pl.ds(kh, 32)].reshape(512, 384)
            got = jnp.dot(act_t[...], rhs, preferred_element_type=F32)
            for kw in range(3):
                tap = 9 * t + 3 * kh + kw
                block = got[:, 128 * kw : 128 * kw + 128].T.reshape(8, 16, 128)
                part_one[:, slot_of(tap)] = block.astype(BF16)
    red_one.pair_send()
    grads = (red_two, red_one)
    for s in range(2):
        red_one.pair_sum(s)
        red_one.first_send(s)
    dpre.frame_wait()
    transposed(one, one_t)
    dpre.windows(1)
    dpre.middle(one_t, out_v)
    for red in grads:
        for s in range(2):
            red.first_sum(s)
            red.second_send(s)
    dpre.bulk_send(0)
    dpre.bulk_send(1)
    dpre.rim_send()
    for red in grads:
        for s in range(2):
            red.second_sum(s)
            red.third_send(s)
    for red in grads:
        for s in range(2):
            red.third_sum(s)
            red.second_gather(s)
    dpre.times_wait()
    dpre.windows(0)
    dpre.windows(2)
    dpre.outer(one_t, out_v)

    def finish(g, _):
        row = 4 * g
        d_vol[pl.ds(row, 4)] = shifted(out_v, row).astype(BF16)
        return 0

    lax.fori_loop(0, 8, finish, 0)
    for red in grads:
        for s in range(2):
            red.first_gather(s)
    for red in grads:
        for s in range(2):
            red.pair_gather(s)
    for red in grads:
        for s in range(2):
            red.finish(s)
            red.drain(s)
    for field in (vol, cot, dpre):
        field.drain()


def scale_kernel(scale, full_one, full_two, d_in, grad_one, grad_two, d_out, buf, sems):
    through = pltpu.make_async_copy(d_in, d_out, sems.at[2])
    through.start()
    for g, (full, grad) in enumerate(((full_two, grad_two), (full_one, grad_one))):

        def step(tap, _):
            tiles = full[:, tap + 2 * (tap // 14)].astype(F32) * scale
            buf[g, tap] = tiles.reshape(128, 128)
            pltpu.make_async_copy(buf.at[g, tap], grad.at[tap], sems.at[g]).start()
            return 0

        lax.fori_loop(0, 27, step, 0)
    through.wait()
    wait_bytes(buf.at[0], sems.at[0])
    wait_bytes(buf.at[1], sems.at[1])


def in_hbm(array):
    return pltpu.with_memory_space_constraint(array, pltpu.HBM)


def body(volume, cotangent, kernel_one, kernel_two):
    total_cells = (
        volume.shape[0]
        * volume.shape[1]
        * volume.shape[2]
        * lax.axis_size("ta")
        * lax.axis_size("ha")
        * lax.axis_size("wa")
    )
    scale = float(1.0 / np.sqrt(np.float32(total_cells)))
    full = jax.ShapeDtypeStruct((8, 32, 16, 128), BF16)
    taps = pltpu.VMEM((27, 128, 128), BF16)
    d_volume, full_one, full_two = pl.pallas_call(
        block_kernel,
        out_shape=(jax.ShapeDtypeStruct((32, 16, 128), BF16), full, full),
        in_specs=[pl.BlockSpec(memory_space=pltpu.HBM)] * 4,
        out_specs=[pl.BlockSpec(memory_space=pltpu.VMEM)] * 3,
        scratch_shapes=FIELD_SCRATCH * 3
        + [pltpu.VMEM((8, 32, 16, 128), BF16)] * 2
        + REDUCE_SCRATCH * 2
        + [taps] * 4
        + [pltpu.VMEM((34, 16, 384), F32)] * 2
        + [
            pltpu.VMEM((32, 16, 128), F32),
            pltpu.VMEM((32, 16, 128), BF16),
            pltpu.VMEM((128, 512), BF16),
            pltpu.SemaphoreType.DMA((4,)),
        ],
        compiler_params=pltpu.CompilerParams(
            collective_id=0, has_side_effects=True, vmem_limit_bytes=32 * 1024 * 1024
        ),
    )(
        in_hbm(volume.reshape(32, 16, 128)),
        in_hbm(cotangent.reshape(32, 16, 128)),
        in_hbm(kernel_one.reshape(27, 128, 128)),
        in_hbm(kernel_two.reshape(27, 128, 128)),
    )
    grad = jax.ShapeDtypeStruct((27, 128, 128), F32)
    grad_one, grad_two, d_volume = pl.pallas_call(
        functools.partial(scale_kernel, scale),
        out_shape=(grad, grad, jax.ShapeDtypeStruct((32, 16, 128), BF16)),
        in_specs=[pl.BlockSpec(memory_space=pltpu.VMEM)] * 3,
        out_specs=[pl.BlockSpec(memory_space=pl.ANY)] * 3,
        scratch_shapes=[pltpu.VMEM((2, 27, 128, 128), F32), pltpu.SemaphoreType.DMA((3,))],
        compiler_params=pltpu.CompilerParams(vmem_limit_bytes=16 * 1024 * 1024),
    )(full_one, full_two, d_volume)
    return (
        d_volume.reshape(volume.shape),
        grad_one.reshape(kernel_one.shape),
        grad_two.reshape(kernel_two.shape),
    )


def solution(mesh):
    in_specs = (P("ta", "ha", "wa", None), P("ta", "ha", "wa", None), P(), P())
    out_specs = (P("ta", "ha", "wa", None), P(), P())
    return jax.shard_map(body, mesh=mesh, in_specs=in_specs, out_specs=out_specs, check_vma=False)
```

```python
import functools

import jax
import jax.numpy as jnp
import numpy as np
from jax import lax
from jax.experimental import pallas as pl
from jax.experimental.pallas import tpu as pltpu
from jax.sharding import PartitionSpec as P

MESH = pl.DeviceIdType.MESH
F32 = jnp.float32
BF16 = jnp.bfloat16


class Place:
    def __init__(self):
        self.ta = lax.axis_index("ta")
        self.ha = lax.axis_index("ha")
        self.wa = lax.axis_index("wa")
        self.core = lax.rem(self.wa, 2)
        self.x = lax.rem(self.ta, 4)
        self.y = self.ha
        self.z = (self.wa // 2) * 2 + self.ta // 4

    def peer_x(self, off):
        to = lax.rem(self.x + off, 4)
        return to, (self.ta - self.x + to, self.ha, self.wa)

    def peer_y(self, off):
        to = lax.rem(self.y + off, 4)
        return to, (self.ta, to, self.wa)

    def peer_z(self, off):
        to = lax.rem(self.z + off, 8)
        return to, (lax.rem(to, 2) * 4 + self.x, self.ha, (to // 2) * 2 + self.core)

    def near(self, dta, dha, dwa):
        return (lax.rem(self.ta + dta + 8, 8), lax.rem(self.ha + dha + 4, 4), lax.rem(self.wa + dwa + 8, 8))

    def twin(self):
        return (self.ta, self.ha, self.wa + 1 - 2 * self.core)


def send(src, dst, send_sem, recv_sem, device):
    pltpu.make_async_remote_copy(
        src_ref=src, dst_ref=dst, send_sem=send_sem, recv_sem=recv_sem,
        device_id=device, device_id_type=MESH,
    ).start()


def wait_bytes(ref, sem):
    pltpu.make_async_copy(ref, ref, sem).wait()


PHASES = 9
ARRIVAL = {1: 5, 2: 7, 3: 8}


class Reduce:
    def __init__(self, place, part, full, land0, sums, land1, tops, land2, thirds, sends, recvs):
        self.at = place
        self.part, self.full = part, full
        self.land0, self.sums, self.land1 = land0, sums, land1
        self.tops, self.land2, self.thirds = tops, land2, thirds
        self.sends, self.recvs = sends, recvs

    def first(self, s, off):
        return self.at.peer_x(off) if s == 0 else self.at.peer_y(off)

    def last(self, s, off):
        return self.at.peer_y(off) if s == 0 else self.at.peer_x(off)

    def mine(self, s):
        return (self.at.x, self.at.y) if s == 0 else (self.at.y, self.at.x)

    def go(self, phase, s, src, dst, device):
        send(src, dst, self.sends.at[phase, s], self.recvs.at[phase, s], device)

    def pair_send(self):
        other = 4 - 4 * self.at.core
        for s in range(2):
            self.go(0, s, self.part.at[pl.ds(other, 4), pl.ds(16 * s, 14)], self.land0.at[s], self.at.twin())

    def pair_sum(self, s):
        own = 4 * self.at.core
        wait_bytes(self.land0.at[s], self.recvs.at[0, s])

        def step(i, _):
            self.sums[s, i] = self.part[own + i, pl.ds(16 * s, 14)] + self.land0[s, i]
            return 0

        lax.fori_loop(0, 4, step, 0)

    def first_send(self, s):
        for off in range(1, 4):
            to, device = self.first(s, off)
            self.go(1, s, self.sums.at[s, to], self.land1.at[s, off - 1], device)

    def first_sum(self, s):
        me, _ = self.mine(s)
        wait_bytes(self.land1.at[s], self.recvs.at[1, s])
        total = self.sums[s, me].astype(F32)
        for j in range(3):
            total = total + self.land1[s, j].astype(F32)
        self.tops[s, pl.ds(0, 14)] = total.astype(BF16)
        self.tops[s, pl.ds(14, 2)] = jnp.zeros((2, 16, 128), BF16)

    def second_send(self, s):
        for off in (4, 3, 5, 2, 6, 1, 7):
            to, device = self.at.peer_z(off)
            self.go(2, s, self.tops.at[s, pl.ds(2 * to, 2)], self.land2.at[s, off - 1], device)

    def second_sum(self, s):
        _, me = self.mine(s)
        wait_bytes(self.land2.at[s], self.recvs.at[2, s])
        total = self.tops[s, pl.ds(2 * self.at.z, 2)].astype(F32)
        for j in range(7):
            total = total + self.land2[s, j].astype(F32)
        self.thirds[s, me] = total.astype(BF16)

    def third_send(self, s):
        _, me = self.mine(s)
        for off in range(1, 4):
            _, device = self.last(s, off)
            self.go(3, s, self.thirds.at[s, me], self.thirds.at[s, me], device)

    def spot(self, s):
        me, _ = self.mine(s)
        return 4 * self.at.core + me, pl.ds(16 * s + 2 * self.at.z, 2)

    def third_sum(self, s):
        wait_bytes(self.thirds.at[s, pl.ds(0, 3)], self.recvs.at[3, s])
        total = self.thirds[s, 0].astype(F32)
        for j in range(1, 4):
            total = total + self.thirds[s, j].astype(F32)
        row, slots = self.spot(s)
        self.full[row, slots] = total.astype(BF16)

    def second_gather(self, s):
        row, slots = self.spot(s)
        for off in (4, 3, 5, 2, 6, 1, 7):
            _, device = self.at.peer_z(off)
            self.go(4, s, self.full.at[row, slots], self.full.at[row, slots], device)

    def first_gather(self, s):
        me, _ = self.mine(s)
        wait_bytes(self.full.at[0, pl.ds(0, 14)], self.recvs.at[4, s])
        row = 4 * self.at.core + me
        own = self.full.at[row, pl.ds(16 * s, 14)]
        for off in range(1, 4):
            _, device = self.first(s, off)
            self.go(ARRIVAL[off], s, own, own, device)
        self.go(6, s, own, own, self.at.twin())

    def pair_gather(self, s):
        me, _ = self.mine(s)
        for off in (1, 3, 2):
            wait_bytes(self.full.at[0, pl.ds(0, 14)], self.recvs.at[ARRIVAL[off], s])
            row = 4 * self.at.core + lax.rem(me + 4 - off, 4)
            got = self.full.at[row, pl.ds(16 * s, 14)]
            self.go(6, s, got, got, self.at.twin())

    def finish(self, s):
        wait_bytes(self.full.at[pl.ds(0, 4), pl.ds(0, 14)], self.recvs.at[6, s])

    def drain(self, s):
        wait_bytes(self.land0.at[s], self.sends.at[0, s])
        wait_bytes(self.land1.at[s], self.sends.at[1, s])
        wait_bytes(self.land2.at[s], self.sends.at[2, s])
        wait_bytes(self.thirds.at[s, pl.ds(0, 3)], self.sends.at[3, s])
        wait_bytes(self.full.at[0, pl.ds(0, 14)], self.sends.at[4, s])
        for phase in ARRIVAL.values():
            wait_bytes(self.full.at[0, pl.ds(0, 14)], self.sends.at[phase, s])
        wait_bytes(self.full.at[pl.ds(0, 4), pl.ds(0, 14)], self.sends.at[6, s])


REDUCE_SCRATCH = [
    pltpu.VMEM((2, 4, 14, 16, 128), BF16),
    pltpu.VMEM((2, 4, 14, 16, 128), BF16),
    pltpu.VMEM((2, 3, 14, 16, 128), BF16),
    pltpu.VMEM((2, 16, 16, 128), BF16),
    pltpu.VMEM((2, 7, 2, 16, 128), BF16),
    pltpu.VMEM((2, 4, 2, 16, 128), BF16),
    pltpu.SemaphoreType.DMA((PHASES, 2)),
    pltpu.SemaphoreType.DMA((PHASES, 2)),
]


def reduce_peers(place):
    peers = [place.twin()]
    peers += [place.peer_x(off)[1] for off in range(1, 4)]
    peers += [place.peer_y(off)[1] for off in range(1, 4)]
    peers += [place.peer_z(off)[1] for off in range(1, 8)]
    return peers


class Field:
    def __init__(self, place, raw, wide, cols, ends, cols_out, ends_out, win, sends, recvs):
        self.at = place
        self.raw, self.wide = raw, wide
        self.cols, self.ends, self.cols_out, self.ends_out = cols, ends, cols_out, ends_out
        self.win, self.sends, self.recvs = win, sends, recvs

    def stage(self):
        own = self.raw[1, pl.ds(1, 32)].astype(F32)
        self.wide[...] = own.reshape(512, 128)
        self.cols_out[0] = self.wide[pl.ds(0, 32, stride=16), :].astype(BF16)
        self.cols_out[1] = self.wide[pl.ds(15, 32, stride=16), :].astype(BF16)
        self.ends_out[0] = self.wide[pl.ds(0, 1), :]
        self.ends_out[1] = self.wide[pl.ds(496, 1), :]
        self.ends_out[2] = self.wide[pl.ds(15, 1), :]
        self.ends_out[3] = self.wide[pl.ds(511, 1), :]

    def go(self, kind, src, dst, device):
        send(src, dst, self.sends.at[kind], self.recvs.at[kind], device)

    def frame_send(self):
        near = self.at.near
        self.go(0, self.raw.at[1, 1], self.raw.at[1, 33], near(0, -1, 0))
        self.go(0, self.raw.at[1, 32], self.raw.at[1, 0], near(0, 1, 0))
        self.go(1, self.cols_out.at[0], self.cols.at[1, 1], near(0, 0, -1))
        self.go(1, self.cols_out.at[1], self.cols.at[1, 0], near(0, 0, 1))
        self.go(2, self.ends_out.at[0], self.ends.at[1, 3], near(0, -1, -1))
        self.go(2, self.ends_out.at[1], self.ends.at[1, 2], near(0, 1, -1))
        self.go(2, self.ends_out.at[2], self.ends.at[1, 1], near(0, -1, 1))
        self.go(2, self.ends_out.at[3], self.ends.at[1, 0], near(0, 1, 1))

    def bulk_send(self, half):
        near = self.at.near
        rows = pl.ds(1 + 16 * half, 16)
        own = self.raw.at[1, rows]
        self.go(3, own, self.raw.at[0, rows], near(1, 0, 0))
        self.go(3, own, self.raw.at[2, rows], near(-1, 0, 0))

    def frame_wait(self):
        wait_bytes(self.raw.at[1, pl.ds(0, 2)], self.recvs.at[0])
        wait_bytes(self.cols.at[1], self.recvs.at[1])
        wait_bytes(self.ends.at[1], self.recvs.at[2])

    def rim_send(self):
        for frame, step in ((0, 1), (2, -1)):
            device = self.at.near(step, 0, 0)
            self.go(4, self.raw.at[1, 0], self.raw.at[frame, 0], device)
            self.go(4, self.raw.at[1, 33], self.raw.at[frame, 33], device)
            self.go(5, self.cols.at[1], self.cols.at[frame], device)
            self.go(6, self.ends.at[1], self.ends.at[frame], device)

    def times_wait(self):
        wait_bytes(self.raw.at[pl.ds(0, 2), pl.ds(0, 32)], self.recvs.at[3])
        wait_bytes(self.raw.at[0, pl.ds(0, 4)], self.recvs.at[4])
        wait_bytes(self.cols.at[pl.ds(0, 2)], self.recvs.at[5])
        wait_bytes(self.ends.at[pl.ds(0, 2)], self.recvs.at[6])

    def drain(self):
        wait_bytes(self.raw.at[1, pl.ds(0, 2)], self.sends.at[0])
        wait_bytes(self.cols.at[1], self.sends.at[1])
        wait_bytes(self.ends.at[1], self.sends.at[2])
        wait_bytes(self.raw.at[pl.ds(0, 2), pl.ds(0, 32)], self.sends.at[3])
        wait_bytes(self.raw.at[0, pl.ds(0, 4)], self.sends.at[4])
        wait_bytes(self.cols.at[pl.ds(0, 2)], self.sends.at[5])
        wait_bytes(self.ends.at[pl.ds(0, 2)], self.sends.at[6])

    def windows(self, frame):
        spot = lax.broadcasted_iota(jnp.int32, (16, 128), 0)
        at_left, at_right = self.at.wa == 0, self.at.wa == 7

        def line(row, left, right):
            mid = self.raw[frame, row]
            wide = mid.astype(F32)
            left = jnp.where(at_left, 0.0, left)
            right = jnp.where(at_right, 0.0, right)
            before = jnp.where(spot == 0, left, pltpu.roll(wide, 1, 0))
            after = jnp.where(spot == 15, right, pltpu.roll(wide, 15, 0))
            self.win[frame, row, :, pl.ds(0, 128)] = before.astype(BF16)
            self.win[frame, row, :, pl.ds(128, 128)] = mid
            self.win[frame, row, :, pl.ds(256, 128)] = after.astype(BF16)

        def group(g, _):
            start = pl.multiple_of(16 * g, 16)
            left = self.cols[frame, 0, pl.ds(start, 16), :].astype(F32)
            right = self.cols[frame, 1, pl.ds(start, 16), :].astype(F32)
            for r in range(16):
                line(16 * g + r + 1, left[r : r + 1], right[r : r + 1])
            return 0

        lax.fori_loop(0, 2, group, 0)
        line(0, self.ends[frame, 0], self.ends[frame, 2])
        line(33, self.ends[frame, 1], self.ends[frame, 3])
        blank = jnp.zeros((16, 384), BF16)

        @pl.when(self.at.ha == 0)
        def _():
            self.win[frame, 0] = blank

        @pl.when(self.at.ha == 3)
        def _():
            self.win[frame, 33] = blank

        if frame != 1:

            @pl.when(self.at.ta == (0 if frame == 0 else 7))
            def _():
                self.win[frame] = jnp.zeros((34, 16, 384), BF16)

    def taps(self, weights, frame):
        rows = [weights[pl.ds(9 * frame + 3 * kh, 3)].reshape(384, 128) for kh in range(3)]
        return jnp.concatenate(rows, axis=1)

    def beside(self, frame):
        rows = [self.win[frame, pl.ds(kh, 32)].reshape(512, 384) for kh in range(3)]
        return jnp.concatenate(rows, axis=1)

    def middle(self, weights, out):
        lhs = self.win[1].reshape(544, 384)
        out[...] = jnp.dot(lhs, self.taps(weights, 1), preferred_element_type=F32).reshape(34, 16, 384)

    def outer(self, weights, out):
        lhs = jnp.concatenate([self.win[0].reshape(544, 384), self.win[2].reshape(544, 384)], axis=1)
        rhs = jnp.concatenate([self.taps(weights, 0), self.taps(weights, 2)], axis=0)
        out[...] = out[...] + jnp.dot(lhs, rhs, preferred_element_type=F32).reshape(34, 16, 384)


FIELD_SCRATCH = [
    pltpu.VMEM((3, 34, 16, 128), BF16),
    pltpu.VMEM((512, 128), F32),
    pltpu.VMEM((3, 2, 32, 128), BF16),
    pltpu.VMEM((3, 4, 1, 128), F32),
    pltpu.VMEM((2, 32, 128), BF16),
    pltpu.VMEM((4, 1, 128), F32),
    pltpu.VMEM((3, 34, 16, 384), BF16),
    pltpu.SemaphoreType.DMA((7,)),
    pltpu.SemaphoreType.DMA((7,)),
]


def shifted(out, row):
    return (
        out[pl.ds(row, 4), :, pl.ds(0, 128)]
        + out[pl.ds(row + 1, 4), :, pl.ds(128, 128)]
        + out[pl.ds(row + 2, 4), :, pl.ds(256, 128)]
    )


def slot_of(tap):
    return tap if tap < 14 else tap + 2


def transposed(weights, out):
    def step(n, _):
        out[n] = weights[26 - n].T
        return 0

    lax.fori_loop(0, 27, step, 0)


def block_kernel(vol_hbm, cot_hbm, one_hbm, two_hbm, d_vol, full_one, full_two, *scratch):
    place = Place()
    barrier = pltpu.get_barrier_semaphore()
    others = reduce_peers(place)
    others += [place.near(s, 0, 0) for s in (1, -1)]
    others += [place.near(0, 0, s) for s in (1, -1)]
    others += [place.near(0, a, b) for a in (1, -1) for b in (1, -1)]
    for device in others:
        pl.semaphore_signal(barrier, inc=1, device_id=device, device_id_type=MESH)

    f, r = len(FIELD_SCRATCH), len(REDUCE_SCRATCH)
    vol = Field(place, *scratch[:f])
    cot = Field(place, *scratch[f : 2 * f])
    dpre = Field(place, *scratch[2 * f : 3 * f])
    scratch = scratch[3 * f :]
    part_one, part_two = scratch[0], scratch[1]
    red_two = Reduce(place, part_two, full_two, *scratch[2 : 2 + r])
    red_one = Reduce(place, part_one, full_one, *scratch[2 + r : 2 + 2 * r])
    scratch = scratch[2 + 2 * r :]
    one, two, one_t, two_t, out_v, out_c, gate, act, act_t, local = scratch

    loads = [
        pltpu.make_async_copy(vol_hbm, vol.raw.at[1, pl.ds(1, 32)], local.at[0]),
        pltpu.make_async_copy(cot_hbm, cot.raw.at[1, pl.ds(1, 32)], local.at[1]),
        pltpu.make_async_copy(two_hbm, two, local.at[2]),
        pltpu.make_async_copy(one_hbm, one, local.at[3]),
    ]
    for load in loads:
        load.start()
    part_one[:, 29] = jnp.zeros((8, 16, 128), BF16)
    part_two[:, 29] = jnp.zeros((8, 16, 128), BF16)
    loads[0].wait()
    vol.stage()
    loads[1].wait()
    cot.stage()
    pl.semaphore_wait(barrier, len(others))

    vol.frame_send()
    cot.frame_send()
    vol.bulk_send(0)
    vol.bulk_send(1)
    cot.bulk_send(0)
    loads[2].wait()
    transposed(two, two_t)
    loads[3].wait()
    vol.frame_wait()
    vol.rim_send()
    cot.bulk_send(1)
    cot.frame_wait()
    cot.rim_send()
    vol.windows(1)
    cot.windows(1)
    vol.middle(one, out_v)
    cot.middle(two_t, out_c)

    vol.times_wait()
    vol.windows(0)
    vol.windows(2)
    vol.outer(one, out_v)

    def activate(g, _):
        row = 4 * g
        pre = shifted(out_v, row)
        sig = 1.0 / (1.0 + jnp.exp(-pre))
        act[pl.ds(row, 4)] = (pre * sig).astype(BF16)
        gate[pl.ds(row, 4)] = sig * (1.0 + pre * (1.0 - sig))
        return 0

    lax.fori_loop(0, 8, activate, 0)
    act_t[...] = act[...].reshape(512, 128).T

    def two_taps(t):
        got = jnp.dot(act_t[...], cot.beside(t), preferred_element_type=F32)
        for n in range(9):
            block = got[:, 128 * n : 128 * n + 128].reshape(8, 16, 128)
            part_two[:, slot_of(26 - 9 * t - n)] = block.astype(BF16)

    two_taps(1)
    cot.times_wait()
    cot.windows(0)
    cot.windows(2)
    for t in (0, 2):
        two_taps(t)
    red_two.pair_send()

    cot.outer(two_t, out_c)

    def backward(g, _):
        row = 4 * g
        dpre.raw[1, pl.ds(row + 1, 4)] = (shifted(out_c, row) * gate[pl.ds(row, 4)]).astype(BF16)
        return 0

    lax.fori_loop(0, 8, backward, 0)
    dpre.stage()
    dpre.frame_send()
    act_t[...] = dpre.raw[1, pl.ds(1, 32)].reshape(512, 128).T
    for s in range(2):
        red_two.pair_sum(s)
        red_two.first_send(s)
    for t in range(3):
        got = jnp.dot(act_t[...], vol.beside(t), preferred_element_type=F32)
        for n in range(9):
            block = got[:, 128 * n : 128 * n + 128].T.reshape(8, 16, 128)
            part_one[:, slot_of(9 * t + n)] = block.astype(BF16)
    red_one.pair_send()
    grads = (red_two, red_one)
    for s in range(2):
        red_one.pair_sum(s)
        red_one.first_send(s)
    dpre.frame_wait()
    transposed(one, one_t)
    dpre.windows(1)
    dpre.middle(one_t, out_v)
    for red in grads:
        for s in range(2):
            red.first_sum(s)
            red.second_send(s)
    dpre.bulk_send(0)
    dpre.bulk_send(1)
    dpre.rim_send()
    for red in grads:
        for s in range(2):
            red.second_sum(s)
            red.third_send(s)
    for red in grads:
        for s in range(2):
            red.third_sum(s)
            red.second_gather(s)
    dpre.times_wait()
    dpre.windows(0)
    dpre.windows(2)
    dpre.outer(one_t, out_v)

    def finish(g, _):
        row = 4 * g
        d_vol[pl.ds(row, 4)] = shifted(out_v, row).astype(BF16)
        return 0

    lax.fori_loop(0, 8, finish, 0)
    for red in grads:
        for s in range(2):
            red.first_gather(s)
    for red in grads:
        for s in range(2):
            red.pair_gather(s)
    for red in grads:
        for s in range(2):
            red.finish(s)
            red.drain(s)
    for field in (vol, cot, dpre):
        field.drain()


def scale_kernel(scale, full_one, full_two, d_in, grad_one, grad_two, d_out, buf, sems):
    through = pltpu.make_async_copy(d_in, d_out, sems.at[2])
    through.start()
    for g, (full, grad) in enumerate(((full_two, grad_two), (full_one, grad_one))):

        def step(i, _):
            for tap in (3 * i, 3 * i + 1, 3 * i + 2):
                tiles = full[:, tap + 2 * (tap // 14)].astype(F32) * scale
                buf[g, tap] = tiles.reshape(128, 128)
            three = pl.ds(3 * i, 3)
            pltpu.make_async_copy(buf.at[g, three], grad.at[three], sems.at[g]).start()
            return 0

        lax.fori_loop(0, 9, step, 0)
    through.wait()
    wait_bytes(buf.at[0], sems.at[0])
    wait_bytes(buf.at[1], sems.at[1])


def in_hbm(array):
    return pltpu.with_memory_space_constraint(array, pltpu.HBM)


def body(volume, cotangent, kernel_one, kernel_two):
    total_cells = (
        volume.shape[0]
        * volume.shape[1]
        * volume.shape[2]
        * lax.axis_size("ta")
        * lax.axis_size("ha")
        * lax.axis_size("wa")
    )
    scale = float(1.0 / np.sqrt(np.float32(total_cells)))
    full = jax.ShapeDtypeStruct((8, 32, 16, 128), BF16)
    taps = pltpu.VMEM((27, 128, 128), BF16)
    d_volume, full_one, full_two = pl.pallas_call(
        block_kernel,
        out_shape=(jax.ShapeDtypeStruct((32, 16, 128), BF16), full, full),
        in_specs=[pl.BlockSpec(memory_space=pltpu.HBM)] * 4,
        out_specs=[pl.BlockSpec(memory_space=pltpu.VMEM)] * 3,
        scratch_shapes=FIELD_SCRATCH * 3
        + [pltpu.VMEM((8, 32, 16, 128), BF16)] * 2
        + REDUCE_SCRATCH * 2
        + [taps] * 4
        + [pltpu.VMEM((34, 16, 384), F32)] * 2
        + [
            pltpu.VMEM((32, 16, 128), F32),
            pltpu.VMEM((32, 16, 128), BF16),
            pltpu.VMEM((128, 512), BF16),
            pltpu.SemaphoreType.DMA((4,)),
        ],
        compiler_params=pltpu.CompilerParams(
            collective_id=0, has_side_effects=True, vmem_limit_bytes=32 * 1024 * 1024
        ),
    )(
        in_hbm(volume.reshape(32, 16, 128)),
        in_hbm(cotangent.reshape(32, 16, 128)),
        in_hbm(kernel_one.reshape(27, 128, 128)),
        in_hbm(kernel_two.reshape(27, 128, 128)),
    )
    grad = jax.ShapeDtypeStruct((27, 128, 128), F32)
    grad_one, grad_two, d_volume = pl.pallas_call(
        functools.partial(scale_kernel, scale),
        out_shape=(grad, grad, jax.ShapeDtypeStruct((32, 16, 128), BF16)),
        in_specs=[pl.BlockSpec(memory_space=pltpu.VMEM)] * 3,
        out_specs=[pl.BlockSpec(memory_space=pl.ANY)] * 3,
        scratch_shapes=[pltpu.VMEM((2, 27, 128, 128), F32), pltpu.SemaphoreType.DMA((3,))],
        compiler_params=pltpu.CompilerParams(vmem_limit_bytes=16 * 1024 * 1024),
    )(full_one, full_two, d_volume)
    return (
        d_volume.reshape(volume.shape),
        grad_one.reshape(kernel_one.shape),
        grad_two.reshape(kernel_two.shape),
    )


def solution(mesh):
    in_specs = (P("ta", "ha", "wa", None), P("ta", "ha", "wa", None), P(), P())
    out_specs = (P("ta", "ha", "wa", None), P(), P())
    return jax.shard_map(body, mesh=mesh, in_specs=in_specs, out_specs=out_specs, check_vma=False)
```

```python
import functools

import jax
import jax.numpy as jnp
import numpy as np
from jax import lax
from jax.experimental import pallas as pl
from jax.experimental.pallas import tpu as pltpu
from jax.sharding import PartitionSpec as P

MESH = pl.DeviceIdType.MESH
F32 = jnp.float32
BF16 = jnp.bfloat16


class Place:
    def __init__(self):
        self.ta = lax.axis_index("ta")
        self.ha = lax.axis_index("ha")
        self.wa = lax.axis_index("wa")
        self.core = lax.rem(self.wa, 2)
        self.x = lax.rem(self.ta, 4)
        self.y = self.ha
        self.z = (self.wa // 2) * 2 + self.ta // 4

    def peer_x(self, off):
        to = lax.rem(self.x + off, 4)
        return to, (self.ta - self.x + to, self.ha, self.wa)

    def peer_y(self, off):
        to = lax.rem(self.y + off, 4)
        return to, (self.ta, to, self.wa)

    def peer_z(self, off):
        to = lax.rem(self.z + off, 8)
        return to, (lax.rem(to, 2) * 4 + self.x, self.ha, (to // 2) * 2 + self.core)

    def near(self, dta, dha, dwa):
        return (lax.rem(self.ta + dta + 8, 8), lax.rem(self.ha + dha + 4, 4), lax.rem(self.wa + dwa + 8, 8))

    def twin(self):
        return (self.ta, self.ha, self.wa + 1 - 2 * self.core)


def send(src, dst, send_sem, recv_sem, device):
    pltpu.make_async_remote_copy(
        src_ref=src, dst_ref=dst, send_sem=send_sem, recv_sem=recv_sem,
        device_id=device, device_id_type=MESH,
    ).start()


def wait_bytes(ref, sem):
    pltpu.make_async_copy(ref, ref, sem).wait()


PHASES = 9
ARRIVAL = {1: 5, 2: 7, 3: 8}


class Reduce:
    def __init__(self, place, part, full, land0, sums, land1, tops, land2, thirds, sends, recvs):
        self.at = place
        self.part, self.full = part, full
        self.land0, self.sums, self.land1 = land0, sums, land1
        self.tops, self.land2, self.thirds = tops, land2, thirds
        self.sends, self.recvs = sends, recvs

    def first(self, s, off):
        return self.at.peer_x(off) if s == 0 else self.at.peer_y(off)

    def last(self, s, off):
        return self.at.peer_y(off) if s == 0 else self.at.peer_x(off)

    def mine(self, s):
        return (self.at.x, self.at.y) if s == 0 else (self.at.y, self.at.x)

    def go(self, phase, s, src, dst, device):
        send(src, dst, self.sends.at[phase, s], self.recvs.at[phase, s], device)

    def pair_send(self):
        other = 4 - 4 * self.at.core
        for s in range(2):
            self.go(0, s, self.part.at[pl.ds(other, 4), pl.ds(16 * s, 14)], self.land0.at[s], self.at.twin())

    def pair_sum(self, s):
        own = 4 * self.at.core
        wait_bytes(self.land0.at[s], self.recvs.at[0, s])

        def step(i, _):
            self.sums[s, i] = self.part[own + i, pl.ds(16 * s, 14)] + self.land0[s, i]
            return 0

        lax.fori_loop(0, 4, step, 0)

    def first_send(self, s):
        for off in range(1, 4):
            to, device = self.first(s, off)
            self.go(1, s, self.sums.at[s, to], self.land1.at[s, off - 1], device)

    def first_sum(self, s):
        me, _ = self.mine(s)
        wait_bytes(self.land1.at[s], self.recvs.at[1, s])
        total = self.sums[s, me].astype(F32)
        for j in range(3):
            total = total + self.land1[s, j].astype(F32)
        self.tops[s, pl.ds(0, 14)] = total.astype(BF16)
        self.tops[s, pl.ds(14, 2)] = jnp.zeros((2, 16, 128), BF16)

    def second_send(self, s):
        for off in (4, 3, 5, 2, 6, 1, 7):
            to, device = self.at.peer_z(off)
            self.go(2, s, self.tops.at[s, pl.ds(2 * to, 2)], self.land2.at[s, off - 1], device)

    def second_sum(self, s):
        _, me = self.mine(s)
        wait_bytes(self.land2.at[s], self.recvs.at[2, s])
        total = self.tops[s, pl.ds(2 * self.at.z, 2)].astype(F32)
        for j in range(7):
            total = total + self.land2[s, j].astype(F32)
        self.thirds[s, me] = total.astype(BF16)

    def third_send(self, s):
        _, me = self.mine(s)
        for off in range(1, 4):
            _, device = self.last(s, off)
            self.go(3, s, self.thirds.at[s, me], self.thirds.at[s, me], device)

    def spot(self, s):
        me, _ = self.mine(s)
        return 4 * self.at.core + me, pl.ds(16 * s + 2 * self.at.z, 2)

    def third_sum(self, s):
        wait_bytes(self.thirds.at[s, pl.ds(0, 3)], self.recvs.at[3, s])
        total = self.thirds[s, 0].astype(F32)
        for j in range(1, 4):
            total = total + self.thirds[s, j].astype(F32)
        row, slots = self.spot(s)
        self.full[row, slots] = total.astype(BF16)

    def second_gather(self, s):
        row, slots = self.spot(s)
        for off in (4, 3, 5, 2, 6, 1, 7):
            _, device = self.at.peer_z(off)
            self.go(4, s, self.full.at[row, slots], self.full.at[row, slots], device)

    def first_gather(self, s):
        me, _ = self.mine(s)
        wait_bytes(self.full.at[0, pl.ds(0, 14)], self.recvs.at[4, s])
        row = 4 * self.at.core + me
        own = self.full.at[row, pl.ds(16 * s, 14)]
        for off in range(1, 4):
            _, device = self.first(s, off)
            self.go(ARRIVAL[off], s, own, own, device)
        self.go(6, s, own, own, self.at.twin())

    def pair_gather(self, s):
        me, _ = self.mine(s)
        for off in (1, 3, 2):
            wait_bytes(self.full.at[0, pl.ds(0, 14)], self.recvs.at[ARRIVAL[off], s])
            row = 4 * self.at.core + lax.rem(me + 4 - off, 4)
            got = self.full.at[row, pl.ds(16 * s, 14)]
            self.go(6, s, got, got, self.at.twin())

    def finish(self, s):
        wait_bytes(self.full.at[pl.ds(0, 4), pl.ds(0, 14)], self.recvs.at[6, s])

    def drain(self, s):
        wait_bytes(self.land0.at[s], self.sends.at[0, s])
        wait_bytes(self.land1.at[s], self.sends.at[1, s])
        wait_bytes(self.land2.at[s], self.sends.at[2, s])
        wait_bytes(self.thirds.at[s, pl.ds(0, 3)], self.sends.at[3, s])
        wait_bytes(self.full.at[0, pl.ds(0, 14)], self.sends.at[4, s])
        for phase in ARRIVAL.values():
            wait_bytes(self.full.at[0, pl.ds(0, 14)], self.sends.at[phase, s])
        wait_bytes(self.full.at[pl.ds(0, 4), pl.ds(0, 14)], self.sends.at[6, s])


REDUCE_SCRATCH = [
    pltpu.VMEM((2, 4, 14, 16, 128), BF16),
    pltpu.VMEM((2, 4, 14, 16, 128), BF16),
    pltpu.VMEM((2, 3, 14, 16, 128), BF16),
    pltpu.VMEM((2, 16, 16, 128), BF16),
    pltpu.VMEM((2, 7, 2, 16, 128), BF16),
    pltpu.VMEM((2, 4, 2, 16, 128), BF16),
    pltpu.SemaphoreType.DMA((PHASES, 2)),
    pltpu.SemaphoreType.DMA((PHASES, 2)),
]


def reduce_peers(place):
    peers = [place.twin()]
    peers += [place.peer_x(off)[1] for off in range(1, 4)]
    peers += [place.peer_y(off)[1] for off in range(1, 4)]
    peers += [place.peer_z(off)[1] for off in range(1, 8)]
    return peers


class Field:
    def __init__(self, place, raw, wide, cols, ends, cols_out, ends_out, win, sends, recvs):
        self.at = place
        self.raw, self.wide = raw, wide
        self.cols, self.ends, self.cols_out, self.ends_out = cols, ends, cols_out, ends_out
        self.win, self.sends, self.recvs = win, sends, recvs

    def stage(self):
        own = self.raw[1, pl.ds(1, 32)].astype(F32)
        self.wide[...] = own.reshape(512, 128)
        self.cols_out[0] = self.wide[pl.ds(0, 32, stride=16), :].astype(BF16)
        self.cols_out[1] = self.wide[pl.ds(15, 32, stride=16), :].astype(BF16)
        self.ends_out[0] = self.wide[pl.ds(0, 1), :]
        self.ends_out[1] = self.wide[pl.ds(496, 1), :]
        self.ends_out[2] = self.wide[pl.ds(15, 1), :]
        self.ends_out[3] = self.wide[pl.ds(511, 1), :]

    def go(self, kind, src, dst, device):
        send(src, dst, self.sends.at[kind], self.recvs.at[kind], device)

    def frame_send(self):
        near = self.at.near
        self.go(0, self.raw.at[1, 1], self.raw.at[1, 33], near(0, -1, 0))
        self.go(0, self.raw.at[1, 32], self.raw.at[1, 0], near(0, 1, 0))
        self.go(1, self.cols_out.at[0], self.cols.at[1, 1], near(0, 0, -1))
        self.go(1, self.cols_out.at[1], self.cols.at[1, 0], near(0, 0, 1))
        self.go(2, self.ends_out.at[0], self.ends.at[1, 3], near(0, -1, -1))
        self.go(2, self.ends_out.at[1], self.ends.at[1, 2], near(0, 1, -1))
        self.go(2, self.ends_out.at[2], self.ends.at[1, 1], near(0, -1, 1))
        self.go(2, self.ends_out.at[3], self.ends.at[1, 0], near(0, 1, 1))

    def bulk_send(self, half):
        near = self.at.near
        rows = pl.ds(1 + 16 * half, 16)
        own = self.raw.at[1, rows]
        self.go(3, own, self.raw.at[0, rows], near(1, 0, 0))
        self.go(3, own, self.raw.at[2, rows], near(-1, 0, 0))

    def frame_wait(self):
        wait_bytes(self.raw.at[1, pl.ds(0, 2)], self.recvs.at[0])
        wait_bytes(self.cols.at[1], self.recvs.at[1])
        wait_bytes(self.ends.at[1], self.recvs.at[2])

    def rim_send(self):
        for frame, step in ((0, 1), (2, -1)):
            device = self.at.near(step, 0, 0)
            self.go(4, self.raw.at[1, 0], self.raw.at[frame, 0], device)
            self.go(4, self.raw.at[1, 33], self.raw.at[frame, 33], device)
            self.go(5, self.cols.at[1], self.cols.at[frame], device)
            self.go(6, self.ends.at[1], self.ends.at[frame], device)

    def times_wait(self):
        wait_bytes(self.raw.at[pl.ds(0, 2), pl.ds(0, 32)], self.recvs.at[3])
        wait_bytes(self.raw.at[0, pl.ds(0, 4)], self.recvs.at[4])
        wait_bytes(self.cols.at[pl.ds(0, 2)], self.recvs.at[5])
        wait_bytes(self.ends.at[pl.ds(0, 2)], self.recvs.at[6])

    def drain(self):
        wait_bytes(self.raw.at[1, pl.ds(0, 2)], self.sends.at[0])
        wait_bytes(self.cols.at[1], self.sends.at[1])
        wait_bytes(self.ends.at[1], self.sends.at[2])
        wait_bytes(self.raw.at[pl.ds(0, 2), pl.ds(0, 32)], self.sends.at[3])
        wait_bytes(self.raw.at[0, pl.ds(0, 4)], self.sends.at[4])
        wait_bytes(self.cols.at[pl.ds(0, 2)], self.sends.at[5])
        wait_bytes(self.ends.at[pl.ds(0, 2)], self.sends.at[6])

    def windows(self, frame):
        spot = lax.broadcasted_iota(jnp.int32, (16, 128), 0)
        at_left, at_right = self.at.wa == 0, self.at.wa == 7

        def line(row, left, right):
            mid = self.raw[frame, row]
            wide = mid.astype(F32)
            left = jnp.where(at_left, 0.0, left)
            right = jnp.where(at_right, 0.0, right)
            before = jnp.where(spot == 0, left, pltpu.roll(wide, 1, 0))
            after = jnp.where(spot == 15, right, pltpu.roll(wide, 15, 0))
            self.win[frame, row, :, pl.ds(0, 128)] = before.astype(BF16)
            self.win[frame, row, :, pl.ds(128, 128)] = mid
            self.win[frame, row, :, pl.ds(256, 128)] = after.astype(BF16)

        def group(g, _):
            start = pl.multiple_of(16 * g, 16)
            left = self.cols[frame, 0, pl.ds(start, 16), :].astype(F32)
            right = self.cols[frame, 1, pl.ds(start, 16), :].astype(F32)
            for r in range(16):
                line(16 * g + r + 1, left[r : r + 1], right[r : r + 1])
            return 0

        lax.fori_loop(0, 2, group, 0)
        line(0, self.ends[frame, 0], self.ends[frame, 2])
        line(33, self.ends[frame, 1], self.ends[frame, 3])
        blank = jnp.zeros((16, 384), BF16)

        @pl.when(self.at.ha == 0)
        def _():
            self.win[frame, 0] = blank

        @pl.when(self.at.ha == 3)
        def _():
            self.win[frame, 33] = blank

        if frame != 1:

            @pl.when(self.at.ta == (0 if frame == 0 else 7))
            def _():
                self.win[frame] = jnp.zeros((34, 16, 384), BF16)

    def taps(self, weights, frame):
        rows = [weights[pl.ds(9 * frame + 3 * kh, 3)].reshape(384, 128) for kh in range(3)]
        return jnp.concatenate(rows, axis=1)

    def beside(self, frame):
        rows = [self.win[frame, pl.ds(kh, 32)].reshape(512, 384) for kh in range(3)]
        return jnp.concatenate(rows, axis=1)

    def middle(self, weights, out):
        lhs = self.win[1].reshape(544, 384)
        out[...] = jnp.dot(lhs, self.taps(weights, 1), preferred_element_type=F32).reshape(34, 16, 384)

    def outer(self, weights, out):
        lhs = jnp.concatenate([self.win[0].reshape(544, 384), self.win[2].reshape(544, 384)], axis=1)
        rhs = jnp.concatenate([self.taps(weights, 0), self.taps(weights, 2)], axis=0)
        out[...] = out[...] + jnp.dot(lhs, rhs, preferred_element_type=F32).reshape(34, 16, 384)


FIELD_SCRATCH = [
    pltpu.VMEM((3, 34, 16, 128), BF16),
    pltpu.VMEM((512, 128), F32),
    pltpu.VMEM((3, 2, 32, 128), BF16),
    pltpu.VMEM((3, 4, 1, 128), F32),
    pltpu.VMEM((2, 32, 128), BF16),
    pltpu.VMEM((4, 1, 128), F32),
    pltpu.VMEM((3, 34, 16, 384), BF16),
    pltpu.SemaphoreType.DMA((7,)),
    pltpu.SemaphoreType.DMA((7,)),
]


def shifted(out, row):
    return (
        out[pl.ds(row, 4), :, pl.ds(0, 128)]
        + out[pl.ds(row + 1, 4), :, pl.ds(128, 128)]
        + out[pl.ds(row + 2, 4), :, pl.ds(256, 128)]
    )


def slot_of(tap):
    return tap if tap < 14 else tap + 2


def transposed(weights, out):
    def step(n, _):
        out[n] = weights[26 - n].T
        return 0

    lax.fori_loop(0, 27, step, 0)


def block_kernel(vol_hbm, cot_hbm, one_hbm, two_hbm, d_vol, full_one, full_two, *scratch):
    place = Place()
    barrier = pltpu.get_barrier_semaphore()
    others = reduce_peers(place)
    others += [place.near(s, 0, 0) for s in (1, -1)]
    others += [place.near(0, 0, s) for s in (1, -1)]
    others += [place.near(0, a, b) for a in (1, -1) for b in (1, -1)]
    for device in others:
        pl.semaphore_signal(barrier, inc=1, device_id=device, device_id_type=MESH)

    f, r = len(FIELD_SCRATCH), len(REDUCE_SCRATCH)
    vol = Field(place, *scratch[:f])
    cot = Field(place, *scratch[f : 2 * f])
    dpre = Field(place, *scratch[2 * f : 3 * f])
    scratch = scratch[3 * f :]
    part_one, part_two = scratch[0], scratch[1]
    red_two = Reduce(place, part_two, full_two, *scratch[2 : 2 + r])
    red_one = Reduce(place, part_one, full_one, *scratch[2 + r : 2 + 2 * r])
    scratch = scratch[2 + 2 * r :]
    one, two, one_t, two_t, out_v, out_c, gate, act, act_t, local = scratch

    loads = [
        pltpu.make_async_copy(vol_hbm, vol.raw.at[1, pl.ds(1, 32)], local.at[0]),
        pltpu.make_async_copy(cot_hbm, cot.raw.at[1, pl.ds(1, 32)], local.at[1]),
        pltpu.make_async_copy(two_hbm, two, local.at[2]),
        pltpu.make_async_copy(one_hbm, one, local.at[3]),
    ]
    for load in loads:
        load.start()
    part_one[:, 29] = jnp.zeros((8, 16, 128), BF16)
    part_two[:, 29] = jnp.zeros((8, 16, 128), BF16)
    loads[0].wait()
    vol.stage()
    loads[1].wait()
    cot.stage()
    pl.semaphore_wait(barrier, len(others))

    vol.frame_send()
    cot.frame_send()
    vol.bulk_send(0)
    vol.bulk_send(1)
    cot.bulk_send(0)
    loads[2].wait()
    transposed(two, two_t)
    loads[3].wait()
    vol.frame_wait()
    vol.rim_send()
    cot.bulk_send(1)
    cot.frame_wait()
    cot.rim_send()
    vol.windows(1)
    cot.windows(1)
    vol.middle(one, out_v)
    cot.middle(two_t, out_c)

    vol.times_wait()
    vol.windows(0)
    vol.windows(2)
    vol.outer(one, out_v)

    def activate(g, _):
        row = 4 * g
        pre = shifted(out_v, row)
        sig = 1.0 / (1.0 + jnp.exp(-pre))
        act[pl.ds(row, 4)] = (pre * sig).astype(BF16)
        gate[pl.ds(row, 4)] = sig * (1.0 + pre * (1.0 - sig))
        return 0

    lax.fori_loop(0, 8, activate, 0)
    act_t[...] = act[...].reshape(512, 128).T

    def two_taps(t):
        got = jnp.dot(act_t[...], cot.beside(t), preferred_element_type=F32)
        for n in range(9):
            block = got[:, 128 * n : 128 * n + 128].reshape(8, 16, 128)
            part_two[:, slot_of(26 - 9 * t - n)] = block.astype(BF16)

    two_taps(1)
    cot.times_wait()
    cot.windows(0)
    cot.windows(2)
    for t in (0, 2):
        two_taps(t)
    red_two.pair_send()

    cot.outer(two_t, out_c)

    def backward(g, _):
        row = 4 * g
        dpre.raw[1, pl.ds(row + 1, 4)] = (shifted(out_c, row) * gate[pl.ds(row, 4)]).astype(BF16)
        return 0

    lax.fori_loop(0, 8, backward, 0)
    dpre.stage()
    dpre.frame_send()
    act_t[...] = dpre.raw[1, pl.ds(1, 32)].reshape(512, 128).T
    for s in range(2):
        red_two.pair_sum(s)
        red_two.first_send(s)
    for t in range(3):
        got = jnp.dot(act_t[...], vol.beside(t), preferred_element_type=F32)
        for n in range(9):
            block = got[:, 128 * n : 128 * n + 128].T.reshape(8, 16, 128)
            part_one[:, slot_of(9 * t + n)] = block.astype(BF16)
    red_one.pair_send()
    grads = (red_two, red_one)
    for s in range(2):
        red_one.pair_sum(s)
        red_one.first_send(s)
    dpre.frame_wait()
    transposed(one, one_t)
    dpre.windows(1)
    dpre.middle(one_t, out_v)
    for red in grads:
        for s in range(2):
            red.first_sum(s)
            red.second_send(s)
    dpre.bulk_send(0)
    dpre.bulk_send(1)
    dpre.rim_send()
    for red in grads:
        for s in range(2):
            red.second_sum(s)
            red.third_send(s)
    for red in grads:
        for s in range(2):
            red.third_sum(s)
            red.second_gather(s)
    for red in grads:
        for s in range(2):
            red.first_gather(s)
    dpre.times_wait()
    dpre.windows(0)
    dpre.windows(2)
    dpre.outer(one_t, out_v)

    def finish(g, _):
        row = 4 * g
        d_vol[pl.ds(row, 4)] = shifted(out_v, row).astype(BF16)
        return 0

    lax.fori_loop(0, 8, finish, 0)
    for red in grads:
        for s in range(2):
            red.pair_gather(s)
    for red in grads:
        for s in range(2):
            red.finish(s)
            red.drain(s)
    for field in (vol, cot, dpre):
        field.drain()


def scale_kernel(scale, full_one, full_two, d_in, grad_one, grad_two, d_out, buf, sems):
    through = pltpu.make_async_copy(d_in, d_out, sems.at[2])
    through.start()
    for g, (full, grad) in enumerate(((full_two, grad_two), (full_one, grad_one))):

        def step(i, _):
            for tap in (3 * i, 3 * i + 1, 3 * i + 2):
                tiles = full[:, tap + 2 * (tap // 14)].astype(F32) * scale
                buf[g, tap] = tiles.reshape(128, 128)
            three = pl.ds(3 * i, 3)
            pltpu.make_async_copy(buf.at[g, three], grad.at[three], sems.at[g]).start()
            return 0

        lax.fori_loop(0, 9, step, 0)
    through.wait()
    wait_bytes(buf.at[0], sems.at[0])
    wait_bytes(buf.at[1], sems.at[1])


def in_hbm(array):
    return pltpu.with_memory_space_constraint(array, pltpu.HBM)


def body(volume, cotangent, kernel_one, kernel_two):
    total_cells = (
        volume.shape[0]
        * volume.shape[1]
        * volume.shape[2]
        * lax.axis_size("ta")
        * lax.axis_size("ha")
        * lax.axis_size("wa")
    )
    scale = float(1.0 / np.sqrt(np.float32(total_cells)))
    full = jax.ShapeDtypeStruct((8, 32, 16, 128), BF16)
    taps = pltpu.VMEM((27, 128, 128), BF16)
    d_volume, full_one, full_two = pl.pallas_call(
        block_kernel,
        out_shape=(jax.ShapeDtypeStruct((32, 16, 128), BF16), full, full),
        in_specs=[pl.BlockSpec(memory_space=pltpu.HBM)] * 4,
        out_specs=[pl.BlockSpec(memory_space=pltpu.VMEM)] * 3,
        scratch_shapes=FIELD_SCRATCH * 3
        + [pltpu.VMEM((8, 32, 16, 128), BF16)] * 2
        + REDUCE_SCRATCH * 2
        + [taps] * 4
        + [pltpu.VMEM((34, 16, 384), F32)] * 2
        + [
            pltpu.VMEM((32, 16, 128), F32),
            pltpu.VMEM((32, 16, 128), BF16),
            pltpu.VMEM((128, 512), BF16),
            pltpu.SemaphoreType.DMA((4,)),
        ],
        compiler_params=pltpu.CompilerParams(
            collective_id=0, has_side_effects=True, vmem_limit_bytes=32 * 1024 * 1024
        ),
    )(
        in_hbm(volume.reshape(32, 16, 128)),
        in_hbm(cotangent.reshape(32, 16, 128)),
        in_hbm(kernel_one.reshape(27, 128, 128)),
        in_hbm(kernel_two.reshape(27, 128, 128)),
    )
    grad = jax.ShapeDtypeStruct((27, 128, 128), F32)
    grad_one, grad_two, d_volume = pl.pallas_call(
        functools.partial(scale_kernel, scale),
        out_shape=(grad, grad, jax.ShapeDtypeStruct((32, 16, 128), BF16)),
        in_specs=[pl.BlockSpec(memory_space=pltpu.VMEM)] * 3,
        out_specs=[pl.BlockSpec(memory_space=pl.ANY)] * 3,
        scratch_shapes=[pltpu.VMEM((2, 27, 128, 128), F32), pltpu.SemaphoreType.DMA((3,))],
        compiler_params=pltpu.CompilerParams(vmem_limit_bytes=16 * 1024 * 1024),
    )(full_one, full_two, d_volume)
    return (
        d_volume.reshape(volume.shape),
        grad_one.reshape(kernel_one.shape),
        grad_two.reshape(kernel_two.shape),
    )


def solution(mesh):
    in_specs = (P("ta", "ha", "wa", None), P("ta", "ha", "wa", None), P(), P())
    out_specs = (P("ta", "ha", "wa", None), P(), P())
    return jax.shard_map(body, mesh=mesh, in_specs=in_specs, out_specs=out_specs, check_vma=False)
```
